512 devices in a mesh: row: 32 (over z, core), vec: 16 (over y, x).
Axes of the slice: x: 4, y: 4, z: 16, core: 2. Of those that a mesh axis runs over, the one named last changes fastest.
Arguments:
- vectors: float32 [32768, 2048], P('row', 'vec'), may hold values from -6 to 6
- reflectors: float32 [3, 32768, 512], P(None, ('row', 'vec')), may hold values from -0.03125 to 0.03125
- triangles: float32 [3, 512, 512], P(None, None, 'vec'), may hold values from -0.04 to 2, as said below
Outputs:
- transformed: float32 [32768, 2048], P('row', 'vec')
The draws below stay inside these ranges and needn't reach their ends.
Inputs may be any that keep to these rules, and one draw needn't show every extreme that they name: Each triangles[k] is upper triangular with a diagonal between 0.5 and 2.
All inputs are finite; a program needn't handle non-finite values.
Results may differ from the reference program's by a relative error of at most 0.0001.
Values sent between devices are 32-bit elements; how exact they have to be, the bound alone decides.
A program may use at most 64 MiB of HBM per device.

```python
import jax
import jax.numpy as jnp
from jax import lax

B = 512
PANELS = 3
ROWS = 32768
EIGS = 2048


def draw_triangles(key, part):
    first, second = jax.random.split(jax.random.fold_in(key, 11))
    upper = jax.random.uniform(first, (PANELS, B, B), jnp.float32, -0.04, 0.04)
    diagonal = jax.random.uniform(second, (PANELS, B), jnp.float32, 1.0, 2.0)
    rowsidx = lax.broadcasted_iota(jnp.int32, (B, B), 0)
    colsidx = lax.broadcasted_iota(jnp.int32, (B, B), 1)
    return jnp.where(rowsidx == colsidx, diagonal[:, :, None], jnp.where(colsidx > rowsidx, upper, 0.0))


def block_scale(own_key, shape, cuts, least, largest):
    factor_of = 1.0
    for axis_at, blocks in cuts:
        heights = jax.random.uniform(jax.random.fold_in(jax.random.fold_in(own_key, 6), axis_at), (blocks,), jnp.float32, least / len(cuts), largest / len(cuts))
        factor_of = factor_of * jnp.repeat(jnp.exp(heights), shape[axis_at] // blocks).reshape((-1,) + (1,) * (len(shape) - 1 - axis_at))
    return factor_of


def gaussian(stream_key, extent, deviation, bound, pieces=(), dtype=jnp.bfloat16):
    drawn = jax.random.normal(stream_key, extent, jnp.float32) * deviation
    if len(pieces) > 0:
        drawn = block_scale(stream_key, extent, pieces, -0.22, 0.18) * drawn
    return jnp.clip(drawn, min=-bound, max=bound).astype(dtype)


def setup_inputs(seed: int = 0) -> dict:
    seeds = jax.random.split(jax.random.key(seed), 4)
    vectors = gaussian(seeds[0], (ROWS, EIGS), 1.0, 6.0, ((0, 32), (1, 16)), jnp.float32)
    reflectors = gaussian(seeds[1], (PANELS, ROWS, B), ROWS ** -0.5, 0.03125, ((1, 512),), jnp.float32)
    triangles = draw_triangles(jax.random.fold_in(seeds[3], 71), 0)
    return {"vectors": vectors, "reflectors": reflectors, "triangles": triangles}


def reference(vectors, reflectors, triangles):
    highest = lax.Precision.HIGHEST
    current = vectors
    for step in range(PANELS):
        panel = PANELS - 1 - step
        section = reflectors[panel]
        projected = lax.dot_general(section, current, (((0,), (0,)), ((), ())), precision=highest, preferred_element_type=jnp.float32)
        coefficients = jnp.dot(triangles[panel], projected, precision=highest, preferred_element_type=jnp.float32)
        current = current - jnp.dot(section, coefficients, precision=highest, preferred_element_type=jnp.float32)
    return current
```

```python
import functools

import jax
import jax.numpy as jnp
from jax import lax
from jax.experimental import pallas as pl
from jax.experimental.pallas import tpu as pltpu
from jax.sharding import Mesh
from jax.sharding import PartitionSpec as P

MESH = pl.DeviceIdType.MESH
VEC = ("y", "x")
ROW = ("z", "core")

SPANS = ((0, 40, 24), (40, 40, 16))
OFFSETS = (0, -1, 1, 2)


def halves(value):
    high = value.astype(jnp.bfloat16)
    low = (value - high.astype(jnp.float32)).astype(jnp.bfloat16)
    return high, low


def product(a, b, dims):
    (a_high, a_low), (b_high, b_low) = a, b
    dot = functools.partial(lax.dot_general, dimension_numbers=(dims, ((), ())), preferred_element_type=jnp.float32)
    return dot(a_high, b_high) + (dot(a_high, b_low) + dot(a_low, b_high))


def kernel(
    x_ref, own_ref, out_ref,
    blocks, other_t, v_high, v_low, t_high, t_low, partial_c, from_core, chip_sum, arrived, coefs,
    gather_send, gather_recv, core_send, core_recv, scatter_send, scatter_recv, spread_send, spread_recv,
):
    panels = own_ref.shape[0]
    rows = own_ref.shape[1] - 16
    z, core = lax.axis_index("z"), lax.axis_index("core")
    y, x = lax.axis_index("y"), lax.axis_index("x")
    depth = lax.axis_size("z")
    place = {"x": x, "y": y}
    me = y * 4 + x

    def step(axis, by):
        return lax.rem(place[axis] + by + 4, 4)

    barrier = pltpu.get_barrier_semaphore()
    for axis in ("x", "y"):
        for by in (1, -1):
            pl.semaphore_signal(barrier, inc=1, device_id={axis: step(axis, by)}, device_id_type=MESH)
    pl.semaphore_signal(barrier, inc=1, device_id={"core": 1 - core}, device_id_type=MESH)
    for by in range(1, depth):
        pl.semaphore_signal(barrier, inc=1, device_id={"z": lax.rem(z + by, depth)}, device_id_type=MESH)
    pl.semaphore_wait(barrier, 5 + depth - 1)

    def block_at(half, first, second):
        first_axis, second_axis = ("x", "y") if half == 0 else ("y", "x")
        at = {first_axis: step(first_axis, first), second_axis: step(second_axis, second)}
        return at["y"] * 4 + at["x"]

    def part_of(half, part):
        start, size, cut = SPANS[half]
        return {"all": (start, size), "plus": (start, cut), "minus": (start + cut, size - cut)}[part]

    def transfer(panel, half, which, part, first, second, second_leg, by, from_own=False):
        index = block_at(half, first, second)
        start, size = part_of(half, part)
        there = blocks.at[panel, index, pl.ds(start, size), :]
        here = own_ref.at[panel, pl.ds(start, size), :] if from_own else there
        axis = ("x", "y")[(half + second_leg) % 2]
        return pltpu.make_async_remote_copy(
            src_ref=here, dst_ref=there,
            send_sem=gather_send.at[panel, half * 20 + which], recv_sem=gather_recv.at[panel, half * 20 + which],
            device_id={axis: step(axis, by)}, device_id_type=MESH,
        )

    sent = []

    def send(*args, **kwargs):
        copy = transfer(*args, **kwargs)
        copy.start()
        sent.append(copy)

    def gather_0(p):
        for h in (0, 1):
            send(p, h, 0, "all", 0, 0, 0, 1, from_own=True)
            send(p, h, 1, "all", 0, 0, 0, -1, from_own=True)
        for h in (0, 1):
            send(p, h, 4, "all", 0, 0, 1, 1, from_own=True)
            send(p, h, 8, "all", 0, 0, 1, -1, from_own=True)
        blocks[p, me] = own_ref[p]

    def gather_1(p):
        for h in (0, 1):
            transfer(p, h, 0, "all", -1, 0, 0, 1).wait_recv()
            send(p, h, 2, "plus", -1, 0, 0, 1)
            transfer(p, h, 1, "all", 1, 0, 0, -1).wait_recv()
            send(p, h, 3, "minus", 1, 0, 0, -1)
        for h in (0, 1):
            for s in (1, 2):
                send(p, h, 4 + s, "all", OFFSETS[s], 0, 1, 1)
                send(p, h, 8 + s, "all", OFFSETS[s], 0, 1, -1)

    def gather_2(p):
        for h in (0, 1):
            transfer(p, h, 2, "plus", 2, 0, 0, 1).wait_recv()
            transfer(p, h, 3, "minus", 2, 0, 0, -1).wait_recv()
            send(p, h, 7, "all", 2, 0, 1, 1)
            send(p, h, 11, "all", 2, 0, 1, -1)

    def gather_3(p):
        for s in range(4):
            for h in (0, 1):
                transfer(p, h, 4 + s, "all", OFFSETS[s], -1, 1, 1).wait_recv()
                send(p, h, 12 + s, "plus", OFFSETS[s], -1, 1, 1)
                transfer(p, h, 8 + s, "all", OFFSETS[s], 1, 1, -1).wait_recv()
                send(p, h, 16 + s, "minus", OFFSETS[s], 1, 1, -1)

    def gather_4(p):
        for s in range(4):
            for h in (0, 1):
                transfer(p, h, 12 + s, "plus", OFFSETS[s], 2, 1, 1).wait_recv()
                transfer(p, h, 16 + s, "minus", OFFSETS[s], 2, 1, -1).wait_recv()

    def to_core(src, dst, which):
        return pltpu.make_async_remote_copy(
            src_ref=src, dst_ref=dst, send_sem=core_send.at[which], recv_sem=core_recv.at[which],
            device_id={"core": 1 - core}, device_id_type=MESH,
        )

    def start(copy):
        copy.start()
        sent.append(copy)

    def factor_copy(p):
        return to_core(blocks.at[p, :, pl.ds(rows, 16), :], other_t.at[p], p)

    def prepare(p):
        start(factor_copy(p))

        @pl.loop(0, 16)
        def _(b):
            high, low = halves(blocks[p, b, 0:rows, :])
            at = pl.ds(pl.multiple_of(b * rows, rows), rows)
            v_high[p, at, :] = high
            v_low[p, at, :] = low
            high, low = halves(blocks[p, b, rows:, :])
            at = pl.ds(pl.multiple_of(b * 32 + core * 16, 16), 16)
            t_high[p, at, :] = high
            t_low[p, at, :] = low

        factor_copy(p).wait_recv()

        @pl.loop(0, 16)
        def _(b):
            high, low = halves(other_t[p, b])
            at = pl.ds(pl.multiple_of(b * 32 + (1 - core) * 16, 16), 16)
            t_high[p, at, :] = high
            t_low[p, at, :] = low

    far_first = sorted(range(1, 16), key=lambda d: -min(d, 16 - d))

    def share_of(at):
        return pl.ds(pl.multiple_of(at // 2 * 8, 8), 8), pl.ds(pl.multiple_of(at % 2 * 256, 256), 256)

    def scatter_copy(p, by):
        to = lax.rem(z + by, depth)
        down, along = share_of(to)
        return pltpu.make_async_remote_copy(
            src_ref=chip_sum.at[p, down, along], dst_ref=arrived.at[p, by],
            send_sem=scatter_send.at[p, by], recv_sem=scatter_recv.at[p, by],
            device_id={"z": to}, device_id_type=MESH,
        )

    def spread_copy(p, by, of):
        down, along = share_of(of)
        at = coefs.at[p, core, down, along]
        return pltpu.make_async_remote_copy(
            src_ref=at, dst_ref=at,
            send_sem=spread_send.at[p, by], recv_sem=spread_recv.at[p, by],
            device_id={"z": lax.rem(z + by, depth)}, device_id_type=MESH,
        )

    def core_sum_copy(p):
        return to_core(partial_c.at[p, 1 - core], from_core.at[p], panels + p)

    def core_spread_copy(p, which):
        return to_core(coefs.at[p, which], coefs.at[p, which], 2 * panels + p)

    last = panels - 1
    gather_0(last)
    out_ref[...] = x_ref[...]
    gather_1(last)
    gather_2(last)
    gather_3(last)
    gather_0(last - 1)
    gather_4(last)
    prepare(last)
    for p in range(last, -1, -1):
        turned = halves(out_ref[...].T)
        projected = product(turned, (v_high[p], v_low[p]), ((1,), (0,)))
        value = product(halves(projected), (t_high[p], t_low[p]), ((1,), (0,)))
        half = value.shape[0] // 2
        partial_c[p, 0] = value[:half]
        partial_c[p, 1] = value[half:]
        start(core_sum_copy(p))
        if p > 0:
            gather_1(p - 1)
        core_sum_copy(p).wait_recv()
        chip_sum[p] = partial_c[p, core] + from_core[p]
        for by in far_first:
            start(scatter_copy(p, by))
        if p > 0:
            gather_2(p - 1)
        down, along = share_of(z)
        total = chip_sum[p, down, along]
        for by in range(1, 16):
            scatter_copy(p, by).wait_recv()
        for by in range(1, 16):
            total = total + arrived[p, by]
        coefs[p, core, down, along] = total
        for by in far_first:
            start(spread_copy(p, by, z))
        if p > 0:
            gather_3(p - 1)
            if p > 1:
                gather_0(p - 2)
            gather_4(p - 1)
            prepare(p - 1)
        for by in range(1, 16):
            spread_copy(p, by, lax.rem(z + depth - by, depth)).wait_recv()
        start(core_spread_copy(p, core))
        core_spread_copy(p, 1 - core).wait_recv()
        turned_c = halves(jnp.concatenate([coefs[p, 0], coefs[p, 1]], axis=0))
        out_ref[...] = out_ref[...] - product((v_high[p], v_low[p]), turned_c, ((1,), (1,)))
    for copy in sent:
        copy.wait_send()


def per_device(vectors, reflectors, triangles):
    panels, rows, width = reflectors.shape
    count = vectors.shape[1]
    everyone = 16 * rows
    turned = jnp.swapaxes(triangles, 1, 2)
    half = turned.shape[1] // 2
    mine = lax.dynamic_slice_in_dim(turned, lax.axis_index("core") * half, half, axis=1)
    own = jnp.concatenate([reflectors, mine], axis=1)
    f32, bf16 = jnp.float32, jnp.bfloat16
    dma = pltpu.SemaphoreType.DMA
    return pl.pallas_call(
        kernel,
        out_shape=jax.ShapeDtypeStruct(vectors.shape, f32),
        in_specs=[pl.BlockSpec(memory_space=pltpu.VMEM)] * 2,
        out_specs=pl.BlockSpec(memory_space=pltpu.VMEM),
        scratch_shapes=[
            pltpu.VMEM((panels, 16, rows + half, width), f32),
            pltpu.VMEM((panels, 16, half, width), f32),
            pltpu.VMEM((panels, everyone, width), bf16),
            pltpu.VMEM((panels, everyone, width), bf16),
            pltpu.VMEM((panels, width, width), bf16),
            pltpu.VMEM((panels, width, width), bf16),
            pltpu.VMEM((panels, 2, count // 2, width), f32),
            pltpu.VMEM((panels, count // 2, width), f32),
            pltpu.VMEM((panels, count // 2, width), f32),
            pltpu.VMEM((panels, 16, 8, 256), f32),
            pltpu.VMEM((panels, 2, count // 2, width), f32),
            dma((panels, 40)), dma((panels, 40)),
            dma((3 * panels,)), dma((3 * panels,)),
            dma((panels, 16)), dma((panels, 16)),
            dma((panels, 16)), dma((panels, 16)),
        ],
        compiler_params=pltpu.CompilerParams(collective_id=0, has_side_effects=True),
    )(vectors, own)


def solution(mesh):
    finer = Mesh(mesh.devices.reshape(16, 2, 4, 4), ("z", "core", "y", "x"))
    placed = (P(ROW, VEC), P(None, ROW + VEC, None), P(None, None, VEC))
    return jax.shard_map(
        per_device, mesh=finer, in_specs=placed, out_specs=P(ROW, VEC), check_vma=False
    )
```

```python
import functools

import jax
import jax.numpy as jnp
from jax import lax
from jax.experimental import pallas as pl
from jax.experimental.pallas import tpu as pltpu
from jax.sharding import Mesh
from jax.sharding import PartitionSpec as P

MESH = pl.DeviceIdType.MESH
VEC = ("y", "x")
ROW = ("z", "core")
STREAMS = 2

SPANS = ((0, 40, 24), (40, 40, 16))
OFFSETS = (0, -1, 1, 2)


def halves(value):
    high = value.astype(jnp.bfloat16)
    low = (value - high.astype(jnp.float32)).astype(jnp.bfloat16)
    return high, low


def product(a, b_high, b_low, contracted):
    a_high, a_low = halves(a)
    count = a.shape[0]
    dot = functools.partial(
        lax.dot_general, dimension_numbers=(((1,), (contracted,)), ((), ())), preferred_element_type=jnp.float32
    )
    both = dot(jnp.concatenate([a_high, a_low], axis=0), b_high)
    return both[:count] + (dot(a_high, b_low) + both[count:])


def kernel(
    x_ref, reflectors_ref, factors_ref, out_ref,
    x_in, x_turned, blocks, other_t, v_high, v_low, t_high, t_low, partial_c, near, near_sum, far, coefs,
    load_sem, entered, gather_send, gather_first, gather_opposite, gather_second, gather_last,
    core_send, factor_recv, near_send, near_recv, far_send, far_recv, spread_send, spread_recv,
):
    panels, rows, width = reflectors_ref.shape
    half_t = factors_ref.shape[1] // 2
    z, core = lax.axis_index("z"), lax.axis_index("core")
    y, x = lax.axis_index("y"), lax.axis_index("x")
    depth = lax.axis_size("z")
    place = {"x": x, "y": y}
    me = y * 4 + x
    last = panels - 1

    def scope(name):
        return jax.named_scope(name)

    def step(axis, by):
        return lax.rem(place[axis] + by + 4, 4)

    def up(by):
        return lax.rem(z + by + depth, depth)

    loads = []
    for p in range(last, -1, -1):
        loads.append(pltpu.make_async_copy(reflectors_ref.at[p], blocks.at[p, me, pl.ds(0, rows), :], load_sem.at[2 * p]))
        loads.append(
            pltpu.make_async_copy(
                factors_ref.at[p, pl.ds(pl.multiple_of(core * half_t, half_t), half_t), :],
                blocks.at[p, me, pl.ds(rows, half_t), :],
                load_sem.at[2 * p + 1],
            )
        )
    load_x = pltpu.make_async_copy(x_ref, x_in, load_sem.at[2 * panels])
    for copy in loads:
        copy.start()
    load_x.start()

    with scope("barrier"):
        barrier = pltpu.get_barrier_semaphore()
        for axis in ("x", "y"):
            for by in (1, -1):
                pl.semaphore_signal(barrier, inc=1, device_id={axis: step(axis, by)}, device_id_type=MESH)
        pl.semaphore_signal(barrier, inc=1, device_id={"core": 1 - core}, device_id_type=MESH)
        for by in (1, -1, 2, -2):
            for other in (core, 1 - core):
                pl.semaphore_signal(barrier, inc=1, device_id={"z": up(by), "core": other}, device_id_type=MESH)
        for copy in loads:
            copy.wait()
        pl.semaphore_wait(barrier, 13)

    def announce(round_):
        for by in (1, -1):
            pl.semaphore_signal(entered.at[round_], inc=1, device_id={"z": up(by * 2 * 2**round_)}, device_id_type=MESH)

    def heard(round_):
        pl.semaphore_wait(entered.at[round_], 2)

    def block_at(half, first, second):
        first_axis, second_axis = ("x", "y") if half == 0 else ("y", "x")
        at = {first_axis: step(first_axis, first), second_axis: step(second_axis, second)}
        return at["y"] * 4 + at["x"]

    def transfer(panel, half, recv, part, first, second, second_leg, by):
        start, size, cut = SPANS[half]
        start, size = {"all": (start, size), "plus": (start, cut), "minus": (start + cut, size - cut)}[part]
        there = blocks.at[panel, block_at(half, first, second), pl.ds(start, size), :]
        axis = ("x", "y")[(half + second_leg) % 2]
        return pltpu.make_async_remote_copy(
            src_ref=there, dst_ref=there, send_sem=gather_send.at[panel], recv_sem=recv,
            device_id={axis: step(axis, by)}, device_id_type=MESH,
        )

    def side(by):
        return 0 if by == 1 else 1

    def first_leg(p, h, by, first=0):
        return transfer(p, h, gather_first.at[p, 2 * h + side(by)], "all", first, 0, 0, by)

    def opposite(p, h, part, by, first):
        return transfer(p, h, gather_opposite.at[p, h], part, first, 0, 0, by)

    def second_leg(p, h, s, by, second=0):
        return transfer(p, h, gather_second.at[p, (h * 4 + s) * 2 + side(by)], "all", OFFSETS[s], second, 1, by)

    def final_leg(p, h, s, part, by):
        return transfer(p, h, gather_last.at[p], part, OFFSETS[s], -by, 1, by)

    def gather_0(p):
        for h in (0, 1):
            for by in (1, -1):
                first_leg(p, h, by).start()
        for h in (0, 1):
            for by in (1, -1):
                second_leg(p, h, 0, by).start()

    def gather_1(p):
        for h in (0, 1):
            first_leg(p, h, 1, -1).wait_recv()
            opposite(p, h, "plus", 1, -1).start()
            first_leg(p, h, -1, 1).wait_recv()
            opposite(p, h, "minus", -1, 1).start()
        for h in (0, 1):
            for s in (1, 2):
                for by in (1, -1):
                    second_leg(p, h, s, by).start()

    def gather_2(p):
        for h in (0, 1):
            opposite(p, h, "all", 1, 2).wait_recv()
            for by in (1, -1):
                second_leg(p, h, 3, by).start()

    def gather_3(p, which):
        for s in which:
            for h in (0, 1):
                for by, part in ((1, "plus"), (-1, "minus")):
                    second_leg(p, h, s, by, -by).wait_recv()
                    final_leg(p, h, s, part, by).start()

    def gather_4(p):
        whole = blocks.at[p, pl.ds(0, 4)]
        pltpu.make_async_remote_copy(
            src_ref=whole, dst_ref=whole, send_sem=gather_send.at[p], recv_sem=gather_last.at[p],
            device_id={"core": 1 - core}, device_id_type=MESH,
        ).wait_recv()

    def to_core(src, dst, send, recv):
        return pltpu.make_async_remote_copy(
            src_ref=src, dst_ref=dst, send_sem=core_send.at[send], recv_sem=recv,
            device_id={"core": 1 - core}, device_id_type=MESH,
        )

    def factor_copy(p):
        return to_core(blocks.at[p, :, pl.ds(rows, half_t), :], other_t.at[p], 0, factor_recv.at[p])

    def prepare(p):
        factor_copy(p).start()

        @pl.loop(0, 16)
        def _(b):
            at = pl.ds(pl.multiple_of(b * rows, rows), rows)
            v_high[p, at, :], v_low[p, at, :] = halves(blocks[p, b, 0:rows, :])
            at = pl.ds(pl.multiple_of(b * 32 + core * 16, 16), 16)
            t_high[p, at, :], t_low[p, at, :] = halves(blocks[p, b, rows:, :])

        factor_copy(p).wait_recv()

        @pl.loop(0, 16)
        def _(b):
            at = pl.ds(pl.multiple_of(b * 32 + (1 - core) * 16, 16), 16)
            t_high[p, at, :], t_low[p, at, :] = halves(other_t[p, b])

    count = x_turned.shape[0] // STREAMS
    NEAR = ((0, 1), (1, 0), (1, 1), (-1, 0), (-1, 1), (2, 0), (2, 1))

    def towards(s, by):
        return by if s % 2 == 0 else -by

    def part_of(chip, core_):
        return pl.ds(pl.multiple_of((lax.rem(chip, 4) * 2 + core_) * (count // 8), count // 8), count // 8)

    def near_copy(p, s, i):
        by, flip = NEAR[i]
        to, other = up(towards(s, by)), core + flip - 2 * core * flip
        return pltpu.make_async_remote_copy(
            src_ref=partial_c.at[p, s, part_of(to, other)], dst_ref=near.at[p, s, i],
            send_sem=near_send.at[0], recv_sem=near_recv.at[p, s],
            device_id={"z": to, "core": other}, device_id_type=MESH,
        )

    def far_copy(p, s, i):
        return pltpu.make_async_remote_copy(
            src_ref=near_sum.at[p, s], dst_ref=far.at[p, s, i],
            send_sem=far_send.at[0], recv_sem=far_recv.at[p, s],
            device_id={"z": up(4 * (i + 1))}, device_id_type=MESH,
        )

    def spread_copy(p, s, i):
        by, flip = NEAR[i]
        own = coefs.at[p, s, part_of(z, core)]
        return pltpu.make_async_remote_copy(
            src_ref=own, dst_ref=own, send_sem=spread_send.at[0], recv_sem=spread_recv.at[p, s],
            device_id={"z": up(-towards(s, by)), "core": core + flip - 2 * core * flip}, device_id_type=MESH,
        )

    def whole_of(ref, send, recv):
        return pltpu.make_async_remote_copy(
            src_ref=ref, dst_ref=ref, send_sem=send, recv_sem=recv, device_id={"core": 1 - core}, device_id_type=MESH
        )

    def columns(s):
        return slice(s * count, (s + 1) * count)

    def project(p, s):
        projected = product(x_turned[columns(s), :], v_high[p], v_low[p], 0)
        partial_c[p, s] = product(projected, t_high[p], t_low[p], 0)
        for i in (5, 6, 1, 2, 3, 4, 0):
            near_copy(p, s, i).start()

    def sum_near(p, s):
        whole_of(near.at[p, s], near_send.at[0], near_recv.at[p, s]).wait_recv()
        total = partial_c[p, s, part_of(z, core)]
        for i in range(7):
            total = total + near[p, s, i]
        near_sum[p, s] = total
        for i in (1, 0, 2):
            far_copy(p, s, i).start()

    def sum_far(p, s):
        whole_of(far.at[p, s], far_send.at[0], far_recv.at[p, s]).wait_recv()
        coefs[p, s, part_of(z, core)] = (near_sum[p, s] + far[p, s, 1]) + (far[p, s, 0] + far[p, s, 2])
        for i in (5, 6, 1, 2, 3, 4, 0):
            spread_copy(p, s, i).start()

    def update(p, s):
        whole_of(near.at[p, s], spread_send.at[0], spread_recv.at[p, s]).wait_recv()
        x_turned[columns(s), :] = x_turned[columns(s), :] - product(coefs[p, s], v_high[p], v_low[p], 1)

    with scope("g0"):
        gather_0(last)
        announce(0)
        load_x.wait()
        x_turned[...] = x_in[...].T
    with scope("g1"):
        gather_1(last)
        heard(0)
        announce(1)
    with scope("g3a"):
        gather_3(last, (0,))
    with scope("g2"):
        gather_2(last)
    with scope("g3"):
        gather_3(last, (1, 2, 3))
        gather_0(last - 1)
        heard(1)
    with scope("g4"):
        gather_4(last)
    with scope("prep"):
        prepare(last)
    for s in range(STREAMS):
        with scope("project"):
            project(last, s)
    for p in range(last, -1, -1):
        if p > 0:
            with scope("g1n"):
                gather_1(p - 1)
        for s in range(STREAMS):
            with scope(f"near{s}"):
                sum_near(p, s)
        if p > 0:
            with scope("g2n"):
                gather_2(p - 1)
            with scope("g3n"):
                gather_3(p - 1, range(4))
                if p > 1:
                    gather_0(p - 2)
        for s in range(STREAMS):
            with scope(f"far{s}"):
                sum_far(p, s)
        if p > 0:
            with scope("g4n"):
                gather_4(p - 1)
            with scope("prepn"):
                prepare(p - 1)
        for s in range(STREAMS):
            with scope(f"update{s}"):
                update(p, s)
            if p > 0:
                with scope("project"):
                    project(p - 1, s)
    with scope("out"):
        x_in[...] = x_turned[...].T
        store = pltpu.make_async_copy(x_in, out_ref, load_sem.at[0])
        store.start()
    with scope("drain"):
        for p in range(panels):
            whole = blocks.at[p, pl.ds(0, 15)]
            pltpu.make_async_remote_copy(
                src_ref=whole, dst_ref=whole, send_sem=gather_send.at[p], recv_sem=gather_last.at[p],
                device_id={"core": 1 - core}, device_id_type=MESH,
            ).wait_send()
        to_core(other_t, other_t, 0, factor_recv.at[0]).wait_send()
        whole_of(near, near_send.at[0], near_recv.at[0, 0]).wait_send()
        whole_of(far, far_send.at[0], far_recv.at[0, 0]).wait_send()
        whole_of(near, spread_send.at[0], spread_recv.at[0, 0]).wait_send()
        store.wait()


def per_device(vectors, reflectors, triangles):
    panels, rows, width = reflectors.shape
    length, count = vectors.shape
    turned = jnp.swapaxes(triangles, 1, 2)
    half = turned.shape[1] // 2
    part = count // STREAMS // 8
    f32, bf16 = jnp.float32, jnp.bfloat16
    dma = pltpu.SemaphoreType.DMA
    return pl.pallas_call(
        kernel,
        out_shape=jax.ShapeDtypeStruct(vectors.shape, f32),
        in_specs=[pl.BlockSpec(memory_space=pl.ANY)] * 3,
        out_specs=pl.BlockSpec(memory_space=pl.ANY),
        scratch_shapes=[
            pltpu.VMEM((length, count), f32),
            pltpu.VMEM((count, length), f32),
            pltpu.VMEM((panels, 16, rows + half, width), f32),
            pltpu.VMEM((panels, 16, half, width), f32),
            pltpu.VMEM((panels, 16 * rows, width), bf16),
            pltpu.VMEM((panels, 16 * rows, width), bf16),
            pltpu.VMEM((panels, width, width), bf16),
            pltpu.VMEM((panels, width, width), bf16),
            pltpu.VMEM((panels, STREAMS, 8 * part, width), f32),
            pltpu.VMEM((panels, STREAMS, 7, part, width), f32),
            pltpu.VMEM((panels, STREAMS, part, width), f32),
            pltpu.VMEM((panels, STREAMS, 3, part, width), f32),
            pltpu.VMEM((panels, STREAMS, 8 * part, width), f32),
            dma((2 * panels + 1,)), pltpu.SemaphoreType.REGULAR((2,)),
            dma((panels,)), dma((panels, 4)), dma((panels, 2)), dma((panels, 16)), dma((panels,)),
            dma((1,)), dma((panels,)), dma((1,)), dma((panels, STREAMS)),
            dma((1,)), dma((panels, STREAMS)), dma((1,)), dma((panels, STREAMS)),
        ],
        compiler_params=pltpu.CompilerParams(collective_id=0, has_side_effects=True),
    )(vectors, reflectors, turned)


def solution(mesh):
    finer = Mesh(mesh.devices.reshape(16, 2, 4, 4), ("z", "core", "y", "x"))
    placed = (P(ROW, VEC), P(None, ROW + VEC, None), P(None, None, VEC))
    return jax.shard_map(
        per_device, mesh=finer, in_specs=placed, out_specs=P(ROW, VEC), check_vma=False
    )
```

```python
import functools

import jax
import jax.numpy as jnp
from jax import lax
from jax.experimental import pallas as pl
from jax.experimental.pallas import tpu as pltpu
from jax.sharding import Mesh
from jax.sharding import PartitionSpec as P

MESH = pl.DeviceIdType.MESH
VEC = ("y", "x")
ROW = ("z", "core")
STREAMS = 2

CARRIED = ((0,), (1, 2), ())
OFFSETS = (0, -1, 1, 2)


def halves(value):
    high = value.astype(jnp.bfloat16)
    low = (value - high.astype(jnp.float32)).astype(jnp.bfloat16)
    return high, low


def product(a, b_high, b_low, contracted):
    a_high, a_low = halves(a)
    count = a.shape[0]
    dot = functools.partial(
        lax.dot_general, dimension_numbers=(((1,), (contracted,)), ((), ())), preferred_element_type=jnp.float32
    )
    both = dot(jnp.concatenate([a_high, a_low], axis=0), b_high)
    return both[:count] + (dot(a_high, b_low) + both[count:])


def kernel(
    x_ref, reflectors_ref, factors_ref, out_ref,
    x_in, x_turned, blocks, other_t, v_high, v_low, t_high, t_low, partial_c, near, near_sum, far, coefs,
    load_sem, entered, gather_send, gather_first, gather_opposite, gather_second, gather_last,
    core_send, factor_recv, near_send, near_recv, far_send, far_recv, spread_send, spread_recv,
):
    panels, rows, width = reflectors_ref.shape
    half_t = factors_ref.shape[1] // 2
    z, core = lax.axis_index("z"), lax.axis_index("core")
    y, x = lax.axis_index("y"), lax.axis_index("x")
    depth = lax.axis_size("z")
    place = {"x": x, "y": y}
    me = y * 4 + x
    last = panels - 1

    def length_of(p):
        return rows + half_t * len(CARRIED[p])

    def scope(name):
        return jax.named_scope(name)

    def step(axis, by):
        return lax.rem(place[axis] + by + 4, 4)

    def up(by):
        return lax.rem(z + by + depth, depth)

    loads = []
    for p in range(last, -1, -1):
        loads.append(pltpu.make_async_copy(reflectors_ref.at[p], blocks.at[p, me, pl.ds(0, rows), :], load_sem.at[2 * p]))
        for i, q in enumerate(CARRIED[p]):
            loads.append(
                pltpu.make_async_copy(
                    factors_ref.at[q, pl.ds(pl.multiple_of(core * half_t, half_t), half_t), :],
                    blocks.at[p, me, pl.ds(rows + i * half_t, half_t), :],
                    load_sem.at[2 * q + 1],
                )
            )
    load_x = pltpu.make_async_copy(x_ref, x_in, load_sem.at[2 * panels])
    for copy in loads:
        copy.start()
    load_x.start()

    with scope("barrier"):
        barrier = pltpu.get_barrier_semaphore()
        for axis in ("x", "y"):
            for by in (1, -1):
                pl.semaphore_signal(barrier, inc=1, device_id={axis: step(axis, by)}, device_id_type=MESH)
        pl.semaphore_signal(barrier, inc=1, device_id={"core": 1 - core}, device_id_type=MESH)
        for by in (1, -1, 2, -2):
            for other in (core, 1 - core):
                pl.semaphore_signal(barrier, inc=1, device_id={"z": up(by), "core": other}, device_id_type=MESH)
        for copy in loads:
            copy.wait()
        pl.semaphore_wait(barrier, 13)

    def announce(round_):
        for by in (1, -1):
            pl.semaphore_signal(entered.at[round_], inc=1, device_id={"z": up(by * 2 * 2**round_)}, device_id_type=MESH)

    def heard(round_):
        pl.semaphore_wait(entered.at[round_], 2)

    def block_at(half, first, second):
        first_axis, second_axis = ("x", "y") if half == 0 else ("y", "x")
        at = {first_axis: step(first_axis, first), second_axis: step(second_axis, second)}
        return at["y"] * 4 + at["x"]

    def transfer(panel, half, recv, part, first, second, second_leg, by):
        size = length_of(panel) // 2
        start, cut = half * size, (size // 2 + 7 * (1 - half)) // 8 * 8
        start, size = {"all": (start, size), "plus": (start, cut), "minus": (start + cut, size - cut)}[part]
        there = blocks.at[panel, block_at(half, first, second), pl.ds(start, size), :]
        axis = ("x", "y")[(half + second_leg) % 2]
        return pltpu.make_async_remote_copy(
            src_ref=there, dst_ref=there, send_sem=gather_send.at[panel], recv_sem=recv,
            device_id={axis: step(axis, by)}, device_id_type=MESH,
        )

    def side(by):
        return 0 if by == 1 else 1

    def first_leg(p, h, by, first=0):
        return transfer(p, h, gather_first.at[p, 2 * h + side(by)], "all", first, 0, 0, by)

    def opposite(p, h, part, by, first):
        return transfer(p, h, gather_opposite.at[p, h], part, first, 0, 0, by)

    def second_leg(p, h, s, by, second=0):
        return transfer(p, h, gather_second.at[p, (h * 4 + s) * 2 + side(by)], "all", OFFSETS[s], second, 1, by)

    def final_leg(p, h, s, part, by):
        return transfer(p, h, gather_last.at[p], part, OFFSETS[s], -by, 1, by)

    def gather_0(p):
        for h in (0, 1):
            for by in (1, -1):
                first_leg(p, h, by).start()
        for h in (0, 1):
            for by in (1, -1):
                second_leg(p, h, 0, by).start()

    def gather_1(p):
        for h in (0, 1):
            first_leg(p, h, 1, -1).wait_recv()
            opposite(p, h, "plus", 1, -1).start()
            first_leg(p, h, -1, 1).wait_recv()
            opposite(p, h, "minus", -1, 1).start()
        for h in (0, 1):
            for s in (1, 2):
                for by in (1, -1):
                    second_leg(p, h, s, by).start()

    def gather_2(p):
        for h in (0, 1):
            opposite(p, h, "all", 1, 2).wait_recv()
            for by in (1, -1):
                second_leg(p, h, 3, by).start()

    def gather_3(p, which):
        for s in which:
            for h in (0, 1):
                for by, part in ((1, "plus"), (-1, "minus")):
                    second_leg(p, h, s, by, -by).wait_recv()
                    final_leg(p, h, s, part, by).start()

    def gather_4(p):
        whole = blocks.at[p, pl.ds(0, 4), pl.ds(0, length_of(p)), :]
        pltpu.make_async_remote_copy(
            src_ref=whole, dst_ref=whole, send_sem=gather_send.at[p], recv_sem=gather_last.at[p],
            device_id={"core": 1 - core}, device_id_type=MESH,
        ).wait_recv()

    def to_core(src, dst, send, recv):
        return pltpu.make_async_remote_copy(
            src_ref=src, dst_ref=dst, send_sem=core_send.at[send], recv_sem=recv,
            device_id={"core": 1 - core}, device_id_type=MESH,
        )

    def factor_copy(p, i, q):
        here = blocks.at[p, :, pl.ds(rows + i * half_t, half_t), :]
        return to_core(here, other_t.at[q], 0, factor_recv.at[q])

    def prepare(p):
        for i, q in enumerate(CARRIED[p]):
            factor_copy(p, i, q).start()

        @pl.loop(0, 16)
        def _(b):
            at = pl.ds(pl.multiple_of(b * rows, rows), rows)
            v_high[p, at, :], v_low[p, at, :] = halves(blocks[p, b, 0:rows, :])
            at = pl.ds(pl.multiple_of(b * 32 + core * 16, 16), 16)
            for i, q in enumerate(CARRIED[p]):
                t_high[q, at, :], t_low[q, at, :] = halves(blocks[p, b, rows + i * half_t : rows + (i + 1) * half_t, :])

        for i, q in enumerate(CARRIED[p]):
            factor_copy(p, i, q).wait_recv()

        if CARRIED[p]:

            @pl.loop(0, 16)
            def _(b):
                at = pl.ds(pl.multiple_of(b * 32 + (1 - core) * 16, 16), 16)
                for q in CARRIED[p]:
                    t_high[q, at, :], t_low[q, at, :] = halves(other_t[q, b])

    count = x_turned.shape[0] // STREAMS
    part = count // 8

    def first_of(quarter):
        return quarter % 2 * 2 + quarter // 2 * 8

    def chip_at(quarter, group, member):
        return lax.rem(first_of(quarter) + group * 4 + member, depth)

    def summing(group):
        return 1 + group // 2

    def group_of(quarter):
        return lax.rem(z - first_of(quarter) + depth, depth) // 4

    my_quarter = lax.rem(z + 3, 4) // 2 + lax.rem(z + 6 * (1 - lax.rem(z, 2)), depth) // 8 * 2
    my_group = group_of(my_quarter)
    my_member = summing(my_group)

    def part_of(quarter, core_):
        return pl.ds(pl.multiple_of((quarter * 2 + core_) * part, part), part)

    def near_copy(p, s, by, other):
        quarter = lax.rem(my_quarter + by, 4)
        group = group_of(quarter)
        member = lax.rem(z - first_of(quarter) + depth, 4)
        return pltpu.make_async_remote_copy(
            src_ref=partial_c.at[p, s, part_of(quarter, other)], dst_ref=near.at[p, s, member * 2 + core],
            send_sem=near_send.at[0], recv_sem=near_recv.at[p, s],
            device_id={"z": chip_at(quarter, group, summing(group)), "core": other}, device_id_type=MESH,
        )

    def far_copy(p, s, by):
        group = lax.rem(my_group + by, 4)
        return pltpu.make_async_remote_copy(
            src_ref=near_sum.at[p, s], dst_ref=far.at[p, s, by - 1],
            send_sem=far_send.at[0], recv_sem=far_recv.at[p, s],
            device_id={"z": chip_at(my_quarter, group, summing(group))}, device_id_type=MESH,
        )

    def spread_copy(p, s, by, other):
        own = coefs.at[p, s, part_of(my_quarter, core)]
        return pltpu.make_async_remote_copy(
            src_ref=own, dst_ref=own, send_sem=spread_send.at[0], recv_sem=spread_recv.at[p, s],
            device_id={"z": chip_at(my_quarter, my_group, lax.rem(my_member + by, 4)), "core": other},
            device_id_type=MESH,
        )

    def each_near(copy, p, s):
        for by in (2, 1, 3):
            copy(p, s, by, core).start()
            copy(p, s, by, 1 - core).start()
        copy(p, s, 0, 1 - core).start()

    def whole_of(ref, send, recv):
        return pltpu.make_async_remote_copy(
            src_ref=ref, dst_ref=ref, send_sem=send, recv_sem=recv, device_id={"core": 1 - core}, device_id_type=MESH
        )

    def columns(s):
        return slice(s * count, (s + 1) * count)

    def project(p, s):
        partial_c[p, s] = product(x_turned[columns(s), :], v_high[p], v_low[p], 0)
        each_near(near_copy, p, s)

    def sum_near(p, s):
        near[p, s, my_member * 2 + core] = partial_c[p, s, part_of(my_quarter, core)]
        whole_of(near.at[p, s, pl.ds(0, 7)], near_send.at[0], near_recv.at[p, s]).wait_recv()
        pairs = [near[p, s, i] + near[p, s, i + 1] for i in range(0, 8, 2)]
        near_sum[p, s] = (pairs[0] + pairs[1]) + (pairs[2] + pairs[3])
        for by in (2, 1, 3):
            far_copy(p, s, by).start()

    def sum_far(p, s):
        whole_of(far.at[p, s], far_send.at[0], far_recv.at[p, s]).wait_recv()
        coefs[p, s, part_of(my_quarter, core)] = (near_sum[p, s] + far[p, s, 1]) + (far[p, s, 0] + far[p, s, 2])
        each_near(spread_copy, p, s)

    def update(p, s):
        whole_of(near.at[p, s, pl.ds(0, 7)], spread_send.at[0], spread_recv.at[p, s]).wait_recv()
        scaled = product(coefs[p, s], t_high[p], t_low[p], 0)
        x_turned[columns(s), :] = x_turned[columns(s), :] - product(scaled, v_high[p], v_low[p], 1)

    with scope("g0"):
        gather_0(last)
        announce(0)
        load_x.wait()
        x_turned[...] = x_in[...].T
    with scope("g1"):
        gather_1(last)
        heard(0)
        announce(1)
    with scope("g2"):
        gather_2(last)
    with scope("g3"):
        gather_3(last, range(4))
        gather_0(last - 1)
        heard(1)
    with scope("g4"):
        gather_4(last)
    with scope("prep"):
        prepare(last)
    for s in range(STREAMS):
        with scope("project"):
            project(last, s)
    for p in range(last, -1, -1):
        if p > 0:
            with scope("g1n"):
                gather_1(p - 1)
        for s in range(STREAMS):
            with scope(f"near{s}"):
                sum_near(p, s)
        if p > 0:
            with scope("g2n"):
                gather_2(p - 1)
            with scope("g3n"):
                gather_3(p - 1, range(4))
                if p > 1:
                    gather_0(p - 2)
        for s in range(STREAMS):
            with scope(f"far{s}"):
                sum_far(p, s)
        if p > 0:
            with scope("g4n"):
                gather_4(p - 1)
            with scope("prepn"):
                prepare(p - 1)
        for s in range(STREAMS):
            with scope(f"update{s}"):
                update(p, s)
            if p > 0:
                with scope("project"):
                    project(p - 1, s)
    with scope("out"):
        out_ref[...] = x_turned[...].T
    with scope("drain"):
        for p in range(panels):
            whole = blocks.at[p, pl.ds(0, 15), pl.ds(0, length_of(p)), :]
            pltpu.make_async_remote_copy(
                src_ref=whole, dst_ref=whole, send_sem=gather_send.at[p], recv_sem=gather_last.at[p],
                device_id={"core": 1 - core}, device_id_type=MESH,
            ).wait_send()
        to_core(other_t, other_t, 0, factor_recv.at[0]).wait_send()
        whole_of(near.at[:, :, pl.ds(0, 7)], near_send.at[0], near_recv.at[0, 0]).wait_send()
        whole_of(far, far_send.at[0], far_recv.at[0, 0]).wait_send()
        whole_of(near.at[:, :, pl.ds(0, 7)], spread_send.at[0], spread_recv.at[0, 0]).wait_send()


def per_device(vectors, reflectors, triangles):
    panels, rows, width = reflectors.shape
    length, count = vectors.shape
    turned = jnp.swapaxes(triangles, 1, 2)
    half = turned.shape[1] // 2
    part = count // STREAMS // 8
    f32, bf16 = jnp.float32, jnp.bfloat16
    dma = pltpu.SemaphoreType.DMA
    return pl.pallas_call(
        kernel,
        out_shape=jax.ShapeDtypeStruct(vectors.shape, f32),
        in_specs=[pl.BlockSpec(memory_space=pltpu.HBM)] * 3,
        out_specs=pl.BlockSpec(memory_space=pltpu.VMEM),
        scratch_shapes=[
            pltpu.VMEM((length, count), f32),
            pltpu.VMEM((count, length), f32),
            pltpu.VMEM((panels, 16, rows + half * max(map(len, CARRIED)), width), f32),
            pltpu.VMEM((panels, 16, half, width), f32),
            pltpu.VMEM((panels, 16 * rows, width), bf16),
            pltpu.VMEM((panels, 16 * rows, width), bf16),
            pltpu.VMEM((panels, width, width), bf16),
            pltpu.VMEM((panels, width, width), bf16),
            pltpu.VMEM((panels, STREAMS, 8 * part, width), f32),
            pltpu.VMEM((panels, STREAMS, 8, part, width), f32),
            pltpu.VMEM((panels, STREAMS, part, width), f32),
            pltpu.VMEM((panels, STREAMS, 3, part, width), f32),
            pltpu.VMEM((panels, STREAMS, 8 * part, width), f32),
            dma((2 * panels + 1,)), pltpu.SemaphoreType.REGULAR((2,)),
            dma((panels,)), dma((panels, 4)), dma((panels, 2)), dma((panels, 16)), dma((panels,)),
            dma((1,)), dma((panels,)), dma((1,)), dma((panels, STREAMS)),
            dma((1,)), dma((panels, STREAMS)), dma((1,)), dma((panels, STREAMS)),
        ],
        compiler_params=pltpu.CompilerParams(collective_id=0, has_side_effects=True, vmem_limit_bytes=36 * 2**20),
    )(*(pltpu.with_memory_space_constraint(a, pltpu.HBM) for a in (vectors, reflectors, turned)))


def solution(mesh):
    finer = Mesh(mesh.devices.reshape(16, 2, 4, 4), ("z", "core", "y", "x"))
    placed = (P(ROW, VEC), P(None, ROW + VEC, None), P(None, None, VEC))
    return jax.shard_map(
        per_device, mesh=finer, in_specs=placed, out_specs=P(ROW, VEC), check_vma=False
    )
```

```python
import functools

import jax
import jax.numpy as jnp
from jax import lax
from jax.experimental import pallas as pl
from jax.experimental.pallas import tpu as pltpu
from jax.sharding import Mesh
from jax.sharding import PartitionSpec as P

MESH = pl.DeviceIdType.MESH
VEC = ("y", "x")
ROW = ("z", "core")
STREAMS = 2
SUMMING = 1

CARRIED = (1, 2, None)
ALONE = 0
OFFSETS = (0, -1, 1, 2)


def halves(value):
    high = value.astype(jnp.bfloat16)
    low = (value - high.astype(jnp.float32)).astype(jnp.bfloat16)
    return high, low


def product(a, b_high, b_low, contracted):
    a_high, a_low = halves(a)
    count = a.shape[0]
    dot = functools.partial(
        lax.dot_general, dimension_numbers=(((1,), (contracted,)), ((), ())), preferred_element_type=jnp.float32
    )
    both = dot(jnp.concatenate([a_high, a_low], axis=0), b_high)
    return both[:count] + (dot(a_high, b_low) + both[count:])


def kernel(
    x_ref, reflectors_ref, factors_ref, out_ref,
    x_in, x_turned, blocks, alone, other_t, v_high, v_low, t_high, t_low, partial_c, near, near_sum, far, coefs,
    load_sem, entered, gather_send, gather_first, gather_opposite, gather_second, gather_last,
    alone_send, alone_recv, core_send, factor_recv, near_send, near_recv, far_send, far_recv, spread_send, spread_recv,
):
    panels, rows, width = reflectors_ref.shape
    half_t = factors_ref.shape[1] // 2
    z, core = lax.axis_index("z"), lax.axis_index("core")
    y, x = lax.axis_index("y"), lax.axis_index("x")
    depth = lax.axis_size("z")
    place = {"x": x, "y": y}
    me = y * 4 + x
    last = panels - 1

    def length_of(p):
        return rows + half_t * (CARRIED[p] is not None)

    def scope(name):
        return jax.named_scope(name)

    def step(axis, by):
        return lax.rem(place[axis] + by + 4, 4)

    def up(by):
        return lax.rem(z + by + depth, depth)

    def own_factor(q, there):
        mine = pl.ds(pl.multiple_of(core * half_t, half_t), half_t)
        return pltpu.make_async_copy(factors_ref.at[q, mine, :], there, load_sem.at[2 * q + 1])

    def load(p):
        copies = [pltpu.make_async_copy(reflectors_ref.at[p], blocks.at[p, me, pl.ds(0, rows), :], load_sem.at[2 * p])]
        if CARRIED[p] is not None:
            copies.append(own_factor(CARRIED[p], blocks.at[p, me, pl.ds(rows, half_t), :]))
        if p == 0:
            copies.append(own_factor(ALONE, alone.at[me]))
        for copy in copies:
            copy.start()
        return copies

    first_load = load(last)
    with scope("barrier"):
        barrier = pltpu.get_barrier_semaphore()
        for axis in ("x", "y"):
            for by in (1, -1):
                pl.semaphore_signal(barrier, inc=1, device_id={axis: step(axis, by)}, device_id_type=MESH)
        for by in (2, -2, 1, -1):
            for other in (core, 1 - core):
                pl.semaphore_signal(barrier, inc=1, device_id={"z": up(by), "core": other}, device_id_type=MESH)
        pl.semaphore_signal(barrier, inc=1, device_id={"core": 1 - core}, device_id_type=MESH)
        for copy in first_load:
            copy.wait()
        pl.semaphore_wait(barrier, 13)

    def announce(round_):
        for by in (1, -1):
            pl.semaphore_signal(entered.at[round_], inc=1, device_id={"z": up(by * 2 * 2**round_)}, device_id_type=MESH)

    def heard(round_):
        pl.semaphore_wait(entered.at[round_], 2)

    def block_at(half, first, second):
        first_axis, second_axis = ("x", "y") if half == 0 else ("y", "x")
        at = {first_axis: step(first_axis, first), second_axis: step(second_axis, second)}
        return at["y"] * 4 + at["x"]

    def transfer(panel, half, recv, part, first, second, second_leg, by):
        size = length_of(panel) // 2
        start, cut = half * size, (size // 2 + 7 * (1 - half)) // 8 * 8
        start, size = {"all": (start, size), "plus": (start, cut), "minus": (start + cut, size - cut)}[part]
        there = blocks.at[panel, block_at(half, first, second), pl.ds(start, size), :]
        axis = ("x", "y")[(half + second_leg) % 2]
        return pltpu.make_async_remote_copy(
            src_ref=there, dst_ref=there, send_sem=gather_send.at[panel], recv_sem=recv,
            device_id={axis: step(axis, by)}, device_id_type=MESH,
        )

    def side(by):
        return 0 if by == 1 else 1

    def first_leg(p, h, by, first=0):
        return transfer(p, h, gather_first.at[p, 2 * h + side(by)], "all", first, 0, 0, by)

    def opposite(p, h, part, by, first):
        return transfer(p, h, gather_opposite.at[p, h], part, first, 0, 0, by)

    def second_leg(p, h, s, by, second=0):
        return transfer(p, h, gather_second.at[p, (h * 4 + s) * 2 + side(by)], "all", OFFSETS[s], second, 1, by)

    def final_leg(p, h, s, part, by):
        return transfer(p, h, gather_last.at[p], part, OFFSETS[s], -by, 1, by)

    def gather_0(p):
        for h in (0, 1):
            for by in (1, -1):
                first_leg(p, h, by).start()
        for h in (0, 1):
            for by in (1, -1):
                second_leg(p, h, 0, by).start()

    def gather_1(p):
        for h in (0, 1):
            first_leg(p, h, 1, -1).wait_recv()
            opposite(p, h, "plus", 1, -1).start()
            first_leg(p, h, -1, 1).wait_recv()
            opposite(p, h, "minus", -1, 1).start()
        for h in (0, 1):
            for s in (1, 2):
                for by in (1, -1):
                    second_leg(p, h, s, by).start()

    def gather_2(p):
        for h in (0, 1):
            opposite(p, h, "all", 1, 2).wait_recv()
            for by in (1, -1):
                second_leg(p, h, 3, by).start()

    def gather_3(p):
        for s in range(4):
            for h in (0, 1):
                for by, part in ((1, "plus"), (-1, "minus")):
                    second_leg(p, h, s, by, -by).wait_recv()
                    final_leg(p, h, s, part, by).start()

    def gather_4(p):
        whole = blocks.at[p, pl.ds(0, 4), pl.ds(0, length_of(p)), :]
        pltpu.make_async_remote_copy(
            src_ref=whole, dst_ref=whole, send_sem=gather_send.at[p], recv_sem=gather_last.at[p],
            device_id={"core": 1 - core}, device_id_type=MESH,
        ).wait_recv()

    def to_core(src, dst, send, recv):
        return pltpu.make_async_remote_copy(
            src_ref=src, dst_ref=dst, send_sem=core_send.at[send], recv_sem=recv,
            device_id={"core": 1 - core}, device_id_type=MESH,
        )

    def factor_copy(q):
        here = alone if q == ALONE else blocks.at[CARRIED.index(q), :, pl.ds(rows, half_t), :]
        return to_core(here, other_t.at[q], 0, factor_recv.at[q])

    def factor_rows(b, core_):
        return pl.ds(pl.multiple_of(b * 32 + core_ * 16, 16), 16)

    def split_panel(p):
        @pl.loop(0, 16)
        def _(b):
            at = pl.ds(pl.multiple_of(b * rows, rows), rows)
            v_high[p, at, :], v_low[p, at, :] = halves(blocks[p, b, 0:rows, :])

    def split_factor(q):
        @pl.loop(0, 16)
        def _(b):
            mine = alone[b] if q == ALONE else blocks[CARRIED.index(q), b, rows : rows + half_t, :]
            t_high[q, factor_rows(b, core), :], t_low[q, factor_rows(b, core), :] = halves(mine)

        factor_copy(q).wait_recv()

        @pl.loop(0, 16)
        def _(b):
            t_high[q, factor_rows(b, 1 - core), :], t_low[q, factor_rows(b, 1 - core), :] = halves(other_t[q, b])

    def send_alone():
        for dy in range(4):
            for dx in range(4):
                if dy or dx:
                    pltpu.make_async_remote_copy(
                        src_ref=alone.at[me], dst_ref=alone.at[me], send_sem=alone_send.at[0], recv_sem=alone_recv.at[0],
                        device_id={"y": step("y", dy), "x": step("x", dx)}, device_id_type=MESH,
                    ).start()

    def alone_wait():
        others = alone.at[pl.ds(0, 15)]
        return pltpu.make_async_remote_copy(
            src_ref=others, dst_ref=others, send_sem=alone_send.at[0], recv_sem=alone_recv.at[0],
            device_id={"core": 1 - core}, device_id_type=MESH,
        )

    count = x_turned.shape[0] // STREAMS
    part = count // 4

    def first_of(quarter):
        return quarter % 2 * 2 + quarter // 2 * 8

    def chip_at(quarter, group, member):
        return lax.rem(first_of(quarter) + group * 4 + member, depth)

    def summing(group):
        return 1 + group // 2

    def group_of(quarter):
        return lax.rem(z - first_of(quarter) + depth, depth) // 4

    my_quarter = lax.rem(z + 3, 4) // 2 + lax.rem(z + 6 * (1 - lax.rem(z, 2)), depth) // 8 * 2
    my_group = group_of(my_quarter)
    my_member = summing(my_group)

    def part_of(quarter):
        return pl.ds(pl.multiple_of(quarter * part, part), part)

    def near_copy(p, s, by):
        quarter = lax.rem(my_quarter + by, 4)
        group = group_of(quarter)
        member = lax.rem(z - first_of(quarter) + depth, 4)
        return pltpu.make_async_remote_copy(
            src_ref=partial_c.at[p, s, part_of(quarter)], dst_ref=near.at[p, s, member * 2 + core],
            send_sem=near_send.at[0], recv_sem=near_recv.at[p, s],
            device_id={"z": chip_at(quarter, group, summing(group)), "core": SUMMING}, device_id_type=MESH,
        )

    def far_copy(p, s, by):
        group = lax.rem(my_group + by, 4)
        return pltpu.make_async_remote_copy(
            src_ref=near_sum.at[p, s], dst_ref=far.at[p, s, by - 1],
            send_sem=far_send.at[0], recv_sem=far_recv.at[p, s],
            device_id={"z": chip_at(my_quarter, group, summing(group)), "core": SUMMING}, device_id_type=MESH,
        )

    def spread_copy(p, s, by, other):
        own = coefs.at[p, s, part_of(my_quarter)]
        return pltpu.make_async_remote_copy(
            src_ref=own, dst_ref=own, send_sem=spread_send.at[0], recv_sem=spread_recv.at[p, s],
            device_id={"z": chip_at(my_quarter, my_group, lax.rem(my_member + by, 4)), "core": other},
            device_id_type=MESH,
        )

    def whole_of(ref, send, recv):
        return pltpu.make_async_remote_copy(
            src_ref=ref, dst_ref=ref, send_sem=send, recv_sem=recv, device_id={"core": 1 - core}, device_id_type=MESH
        )

    def columns(s):
        return slice(s * count, (s + 1) * count)

    def project(p, s):
        partial_c[p, s] = product(x_turned[columns(s), :], v_high[p], v_low[p], 0)
        for by in (2, 1, 3):
            near_copy(p, s, by).start()

        @pl.when(core != SUMMING)
        def _():
            near_copy(p, s, 0).start()

    def sum_near(p, s):
        @pl.when(core == SUMMING)
        def _():
            near[p, s, my_member * 2 + SUMMING] = partial_c[p, s, part_of(my_quarter)]
            whole_of(near.at[p, s, pl.ds(0, 7)], near_send.at[0], near_recv.at[p, s]).wait_recv()
            pairs = [near[p, s, i] + near[p, s, i + 1] for i in range(0, 8, 2)]
            near_sum[p, s] = (pairs[0] + pairs[1]) + (pairs[2] + pairs[3])
            for by in (2, 1, 3):
                far_copy(p, s, by).start()

    def sum_far(p, s):
        @pl.when(core == SUMMING)
        def _():
            whole_of(far.at[p, s], far_send.at[0], far_recv.at[p, s]).wait_recv()
            coefs[p, s, part_of(my_quarter)] = (near_sum[p, s] + far[p, s, 1]) + (far[p, s, 0] + far[p, s, 2])
            for by in (2, 1, 3):
                spread_copy(p, s, by, 1 - SUMMING).start()
                spread_copy(p, s, by, SUMMING).start()
            spread_copy(p, s, 0, 1 - SUMMING).start()

    def update(p, s):
        @pl.when(core == SUMMING)
        def _():
            whole_of(near.at[p, s, pl.ds(0, 3)], spread_send.at[0], spread_recv.at[p, s]).wait_recv()

        @pl.when(core != SUMMING)
        def _():
            whole_of(near.at[p, s, pl.ds(0, 4)], spread_send.at[0], spread_recv.at[p, s]).wait_recv()

        scaled = product(coefs[p, s], t_high[p], t_low[p], 0)
        x_turned[columns(s), :] = x_turned[columns(s), :] - product(scaled, v_high[p], v_low[p], 1)

    with scope("g0"):
        gather_0(last)
        announce(0)
        load_x = pltpu.make_async_copy(x_ref, x_in, load_sem.at[2 * panels])
        load_x.start()
        later_loads = [copy for p in range(last - 1, -1, -1) for copy in load(p)]
        load_x.wait()
        x_turned[...] = x_in[...].T
    with scope("g1"):
        gather_1(last)
        heard(0)
        announce(1)
    with scope("g2"):
        gather_2(last)
    with scope("g3"):
        gather_3(last)
        for copy in later_loads:
            copy.wait()
        gather_0(last - 1)
        heard(1)
    with scope("g4"):
        gather_4(last)
    with scope("prep"):
        split_panel(last)
    for s in range(STREAMS):
        with scope("project"):
            project(last, s)
    with scope("g1n"):
        gather_1(last - 1)
    for p in range(last, -1, -1):
        if p == 0:
            with scope("alone"):
                alone_wait().wait_recv()
                factor_copy(ALONE).start()
        for s in range(STREAMS):
            with scope(f"near{s}"):
                sum_near(p, s)
        if p > 0:
            with scope("g2n"):
                gather_2(p - 1)
            with scope("g3n"):
                gather_3(p - 1)
                if p > 1:
                    gather_0(p - 2)
                else:
                    send_alone()
        for s in range(STREAMS):
            with scope(f"far{s}"):
                sum_far(p, s)
        if p > 0:
            with scope("g4n"):
                gather_4(p - 1)
                factor_copy(CARRIED[p - 1]).start()
            with scope("prepn"):
                split_panel(p - 1)
        if p > 1:
            with scope("g1n"):
                gather_1(p - 2)
        with scope("factor"):
            split_factor(p)
        for s in range(STREAMS):
            with scope(f"update{s}"):
                update(p, s)
            if p > 0:
                with scope("project"):
                    project(p - 1, s)
    with scope("out"):
        out_ref[...] = x_turned[...].T
    with scope("drain"):
        for p in range(panels):
            whole = blocks.at[p, pl.ds(0, 15), pl.ds(0, length_of(p)), :]
            pltpu.make_async_remote_copy(
                src_ref=whole, dst_ref=whole, send_sem=gather_send.at[p], recv_sem=gather_last.at[p],
                device_id={"core": 1 - core}, device_id_type=MESH,
            ).wait_send()
        to_core(other_t, other_t, 0, factor_recv.at[0]).wait_send()
        alone_wait().wait_send()
        @pl.when(core == SUMMING)
        def _():
            whole_of(near.at[:, :, pl.ds(0, 3)], near_send.at[0], near_recv.at[0, 0]).wait_send()
            whole_of(far, far_send.at[0], far_recv.at[0, 0]).wait_send()
            whole_of(near.at[:, :, pl.ds(0, 7)], spread_send.at[0], spread_recv.at[0, 0]).wait_send()

        @pl.when(core != SUMMING)
        def _():
            whole_of(near.at[:, :, pl.ds(0, 4)], near_send.at[0], near_recv.at[0, 0]).wait_send()


def per_device(vectors, reflectors, triangles):
    panels, rows, width = reflectors.shape
    length, count = vectors.shape
    turned = jnp.swapaxes(triangles, 1, 2)
    half = turned.shape[1] // 2
    part = count // STREAMS // 4
    f32, bf16 = jnp.float32, jnp.bfloat16
    dma = pltpu.SemaphoreType.DMA
    return pl.pallas_call(
        kernel,
        out_shape=jax.ShapeDtypeStruct(vectors.shape, f32),
        in_specs=[pl.BlockSpec(memory_space=pltpu.HBM)] * 3,
        out_specs=pl.BlockSpec(memory_space=pltpu.VMEM),
        scratch_shapes=[
            pltpu.VMEM((length, count), f32),
            pltpu.VMEM((count, length), f32),
            pltpu.VMEM((panels, 16, rows + half, width), f32),
            pltpu.VMEM((16, half, width), f32),
            pltpu.VMEM((panels, 16, half, width), f32),
            pltpu.VMEM((panels, 16 * rows, width), bf16),
            pltpu.VMEM((panels, 16 * rows, width), bf16),
            pltpu.VMEM((panels, width, width), bf16),
            pltpu.VMEM((panels, width, width), bf16),
            pltpu.VMEM((panels, STREAMS, 4 * part, width), f32),
            pltpu.VMEM((panels, STREAMS, 8, part, width), f32),
            pltpu.VMEM((panels, STREAMS, part, width), f32),
            pltpu.VMEM((panels, STREAMS, 3, part, width), f32),
            pltpu.VMEM((panels, STREAMS, 4 * part, width), f32),
            dma((2 * panels + 1,)), pltpu.SemaphoreType.REGULAR((2,)),
            dma((panels,)), dma((panels, 4)), dma((panels, 2)), dma((panels, 16)), dma((panels,)),
            dma((1,)), dma((1,)), dma((1,)), dma((panels,)), dma((1,)), dma((panels, STREAMS)),
            dma((1,)), dma((panels, STREAMS)), dma((1,)), dma((panels, STREAMS)),
        ],
        compiler_params=pltpu.CompilerParams(collective_id=0, has_side_effects=True, vmem_limit_bytes=36 * 2**20),
    )(*(pltpu.with_memory_space_constraint(a, pltpu.HBM) for a in (vectors, reflectors, turned)))


def solution(mesh):
    finer = Mesh(mesh.devices.reshape(16, 2, 4, 4), ("z", "core", "y", "x"))
    placed = (P(ROW, VEC), P(None, ROW + VEC, None), P(None, None, VEC))
    return jax.shard_map(
        per_device, mesh=finer, in_specs=placed, out_specs=P(ROW, VEC), check_vma=False
    )
```

```python
import functools

import jax
import jax.numpy as jnp
from jax import lax
from jax.experimental import pallas as pl
from jax.experimental.pallas import tpu as pltpu
from jax.sharding import Mesh
from jax.sharding import PartitionSpec as P

MESH = pl.DeviceIdType.MESH
VEC = ("y", "x")
ROW = ("z", "core")
STREAMS = 2
SUMMING = 1

CARRIED = (1, 2, None)
ALONE = 0
OFFSETS = (0, -1, 1, 2)


def halves(value):
    high = value.astype(jnp.bfloat16)
    low = (value - high.astype(jnp.float32)).astype(jnp.bfloat16)
    return high, low


def product(a, b_high, b_low, contracted):
    a_high, a_low = halves(a)
    count = a.shape[0]
    dot = functools.partial(
        lax.dot_general, dimension_numbers=(((1,), (contracted,)), ((), ())), preferred_element_type=jnp.float32
    )
    both = dot(jnp.concatenate([a_high, a_low], axis=0), b_high)
    return both[:count] + (dot(a_high, b_low) + both[count:])


def kernel(
    x_ref, reflectors_ref, factors_ref, out_ref,
    x_in, x_turned, blocks, alone, other_t, v_high, v_low, w_high, w_low, t_high, t_low, partial_c, near, near_sum, far, coefs,
    load_sem, entered, gather_send, gather_first, gather_opposite, gather_second, gather_last,
    alone_send, alone_recv, core_send, factor_recv, near_send, near_recv, far_send, far_recv, spread_send, spread_recv,
):
    panels, rows, width = reflectors_ref.shape
    half_t = factors_ref.shape[1] // 2
    z, core = lax.axis_index("z"), lax.axis_index("core")
    y, x = lax.axis_index("y"), lax.axis_index("x")
    depth = lax.axis_size("z")
    place = {"x": x, "y": y}
    me = y * 4 + x
    last = panels - 1

    def length_of(p):
        return rows + half_t * (CARRIED[p] is not None)

    def scope(name):
        return jax.named_scope(name)

    def step(axis, by):
        return lax.rem(place[axis] + by + 4, 4)

    def up(by):
        return lax.rem(z + by + depth, depth)

    def own_factor(q, there):
        mine = pl.ds(pl.multiple_of(core * half_t, half_t), half_t)
        return pltpu.make_async_copy(factors_ref.at[q, mine, :], there, load_sem.at[2 * q + 1])

    def load(p):
        copies = [pltpu.make_async_copy(reflectors_ref.at[p], blocks.at[p, me, pl.ds(0, rows), :], load_sem.at[2 * p])]
        if CARRIED[p] is not None:
            copies.append(own_factor(CARRIED[p], blocks.at[p, me, pl.ds(rows, half_t), :]))
        if p == 0:
            copies.append(own_factor(ALONE, alone.at[me]))
        for copy in copies:
            copy.start()
        return copies

    first_load = load(last)
    with scope("barrier"):
        barrier = pltpu.get_barrier_semaphore()
        for axis in ("x", "y"):
            for by in (1, -1, 2):
                pl.semaphore_signal(barrier, inc=1, device_id={axis: step(axis, by)}, device_id_type=MESH)
        for by in (1, -1):
            for other in (core, 1 - core):
                pl.semaphore_signal(barrier, inc=1, device_id={"z": up(by), "core": other}, device_id_type=MESH)
        pl.semaphore_signal(barrier, inc=1, device_id={"core": 1 - core}, device_id_type=MESH)
        for copy in first_load:
            copy.wait()
        pl.semaphore_wait(barrier, 11)

    def announce(round_):
        for by in (1, -1):
            to = up(by * (1, 2, 4)[round_])
            pl.semaphore_signal(entered.at[round_], inc=1, device_id={"z": to}, device_id_type=MESH)
            if round_ == 0:
                pl.semaphore_signal(entered.at[0], inc=1, device_id={"z": to, "core": 1 - core}, device_id_type=MESH)

    def heard(round_):
        pl.semaphore_wait(entered.at[round_], 4 if round_ == 0 else 2)

    def block_at(half, first, second):
        first_axis, second_axis = ("x", "y") if half == 0 else ("y", "x")
        at = {first_axis: step(first_axis, first), second_axis: step(second_axis, second)}
        return at["y"] * 4 + at["x"]

    def transfer(panel, half, recv, part, first, second, second_leg, by):
        size = length_of(panel) // 2
        start, cut = half * size, (size // 2 + 7 * (1 - half)) // 8 * 8
        start, size = {"all": (start, size), "plus": (start, cut), "minus": (start + cut, size - cut)}[part]
        there = blocks.at[panel, block_at(half, first, second), pl.ds(start, size), :]
        axis = ("x", "y")[(half + second_leg) % 2]
        return pltpu.make_async_remote_copy(
            src_ref=there, dst_ref=there, send_sem=gather_send.at[panel], recv_sem=recv,
            device_id={axis: step(axis, by)}, device_id_type=MESH,
        )

    def side(by):
        return 0 if by == 1 else 1

    def first_leg(p, h, by, first=0):
        return transfer(p, h, gather_first.at[p, 2 * h + side(by)], "all", first, 0, 0, by)

    def opposite(p, h, part, by, first):
        return transfer(p, h, gather_opposite.at[p, h], part, first, 0, 0, by)

    def straight(p, h):
        return transfer(p, h, gather_opposite.at[p, h], "all", 0, 0, 0, 2)

    def second_leg(p, h, s, by, second=0):
        return transfer(p, h, gather_second.at[p, (h * 4 + s) * 2 + side(by)], "all", OFFSETS[s], second, 1, by)

    def final_leg(p, h, s, part, by):
        return transfer(p, h, gather_last.at[p], part, OFFSETS[s], -by, 1, by)

    def gather_0(p):
        for h in (0, 1):
            for by in (1, -1):
                first_leg(p, h, by).start()

        @pl.when(core != SUMMING)
        def _():
            for h in (0, 1):
                straight(p, h).start()

        for h in (0, 1):
            for by in (1, -1):
                second_leg(p, h, 0, by).start()

    def gather_1(p):
        for h in (0, 1):
            first_leg(p, h, 1, -1).wait_recv()
            first_leg(p, h, -1, 1).wait_recv()

            @pl.when(core == SUMMING)
            def _():
                opposite(p, h, "plus", 1, -1).start()
                opposite(p, h, "minus", -1, 1).start()

        for h in (0, 1):
            for s in (1, 2):
                for by in (1, -1):
                    second_leg(p, h, s, by).start()

    def gather_2(p):
        for h in (0, 1):
            opposite(p, h, "all", 1, 2).wait_recv()
            for by in (1, -1):
                second_leg(p, h, 3, by).start()

    def gather_3(p):
        for s in range(4):
            for h in (0, 1):
                for by, part in ((1, "plus"), (-1, "minus")):
                    second_leg(p, h, s, by, -by).wait_recv()
                    final_leg(p, h, s, part, by).start()

    def gather_4(p):
        whole = blocks.at[p, pl.ds(0, 4), pl.ds(0, length_of(p)), :]
        pltpu.make_async_remote_copy(
            src_ref=whole, dst_ref=whole, send_sem=gather_send.at[p], recv_sem=gather_last.at[p],
            device_id={"core": 1 - core}, device_id_type=MESH,
        ).wait_recv()

    def to_core(src, dst, send, recv):
        return pltpu.make_async_remote_copy(
            src_ref=src, dst_ref=dst, send_sem=core_send.at[send], recv_sem=recv,
            device_id={"core": 1 - core}, device_id_type=MESH,
        )

    def factor_copy(q):
        here = alone if q == ALONE else blocks.at[CARRIED.index(q), :, pl.ds(rows, half_t), :]
        return to_core(here, other_t.at[q], 0, factor_recv.at[q])

    def factor_rows(b, core_):
        return pl.ds(pl.multiple_of(b * 32 + core_ * 16, 16), 16)

    def split_panel(p):
        @pl.loop(0, 16)
        def _(b):
            at = pl.ds(pl.multiple_of(b * rows, rows), rows)
            v_high[p, at, :], v_low[p, at, :] = halves(blocks[p, b, 0:rows, :])

    def turn_panel(p):
        @pl.loop(0, 8)
        def _(i):
            at = pl.ds(pl.multiple_of(i * 2 * rows, 2 * rows), 2 * rows)
            two = jnp.concatenate([blocks[p, 2 * i, 0:rows, :], blocks[p, 2 * i + 1, 0:rows, :]], axis=0)
            w_high[p, :, at], w_low[p, :, at] = halves(two.T)

    def split_factor(q):
        @pl.loop(0, 16)
        def _(b):
            mine = alone[b] if q == ALONE else blocks[CARRIED.index(q), b, rows : rows + half_t, :]
            t_high[q, factor_rows(b, core), :], t_low[q, factor_rows(b, core), :] = halves(mine)

        factor_copy(q).wait_recv()

        @pl.loop(0, 16)
        def _(b):
            t_high[q, factor_rows(b, 1 - core), :], t_low[q, factor_rows(b, 1 - core), :] = halves(other_t[q, b])

    def send_alone():
        for dy in range(4):
            for dx in range(4):
                if dy or dx:
                    pltpu.make_async_remote_copy(
                        src_ref=alone.at[me], dst_ref=alone.at[me], send_sem=alone_send.at[0], recv_sem=alone_recv.at[0],
                        device_id={"y": step("y", dy), "x": step("x", dx)}, device_id_type=MESH,
                    ).start()

    def alone_wait():
        others = alone.at[pl.ds(0, 15)]
        return pltpu.make_async_remote_copy(
            src_ref=others, dst_ref=others, send_sem=alone_send.at[0], recv_sem=alone_recv.at[0],
            device_id={"core": 1 - core}, device_id_type=MESH,
        )

    count = x_turned.shape[0] // STREAMS
    part = count // 4

    def first_of(quarter):
        return quarter % 2 * 2 + quarter // 2 * 8

    def chip_at(quarter, group, member):
        return lax.rem(first_of(quarter) + group * 4 + member, depth)

    def summing(group):
        return 1 + group // 2

    def group_of(quarter):
        return lax.rem(z - first_of(quarter) + depth, depth) // 4

    my_quarter = lax.rem(z + 3, 4) // 2 + lax.rem(z + 6 * (1 - lax.rem(z, 2)), depth) // 8 * 2
    my_group = group_of(my_quarter)
    my_member = summing(my_group)

    def part_of(quarter):
        return pl.ds(pl.multiple_of(quarter * part, part), part)

    def near_copy(p, s, by):
        quarter = lax.rem(my_quarter + by, 4)
        group = group_of(quarter)
        member = lax.rem(z - first_of(quarter) + depth, 4)
        return pltpu.make_async_remote_copy(
            src_ref=partial_c.at[p, s, part_of(quarter)], dst_ref=near.at[p, s, member * 2 + core],
            send_sem=near_send.at[0], recv_sem=near_recv.at[p, s],
            device_id={"z": chip_at(quarter, group, summing(group)), "core": SUMMING}, device_id_type=MESH,
        )

    def far_copy(p, s, by):
        group = lax.rem(my_group + by, 4)
        return pltpu.make_async_remote_copy(
            src_ref=near_sum.at[p, s], dst_ref=far.at[p, s, by - 1],
            send_sem=far_send.at[0], recv_sem=far_recv.at[p, s],
            device_id={"z": chip_at(my_quarter, group, summing(group)), "core": SUMMING}, device_id_type=MESH,
        )

    def spread_copy(p, s, by, other):
        own = coefs.at[p, s, part_of(my_quarter)]
        return pltpu.make_async_remote_copy(
            src_ref=own, dst_ref=own, send_sem=spread_send.at[0], recv_sem=spread_recv.at[p, s],
            device_id={"z": chip_at(my_quarter, my_group, lax.rem(my_member + by, 4)), "core": other},
            device_id_type=MESH,
        )

    def whole_of(ref, send, recv):
        return pltpu.make_async_remote_copy(
            src_ref=ref, dst_ref=ref, send_sem=send, recv_sem=recv, device_id={"core": 1 - core}, device_id_type=MESH
        )

    def columns(s):
        return slice(s * count, (s + 1) * count)

    def project(p, s):
        partial_c[p, s] = product(x_turned[columns(s), :], v_high[p], v_low[p], 0)
        for by in (2, 1, 3):
            near_copy(p, s, by).start()

        @pl.when(core != SUMMING)
        def _():
            near_copy(p, s, 0).start()

    def sum_near(p, s):
        @pl.when(core == SUMMING)
        def _():
            near[p, s, my_member * 2 + SUMMING] = partial_c[p, s, part_of(my_quarter)]
            whole_of(near.at[p, s, pl.ds(0, 7)], near_send.at[0], near_recv.at[p, s]).wait_recv()
            pairs = [near[p, s, i] + near[p, s, i + 1] for i in range(0, 8, 2)]
            near_sum[p, s] = (pairs[0] + pairs[1]) + (pairs[2] + pairs[3])
            for by in (2, 1, 3):
                far_copy(p, s, by).start()

    def sum_far(p, s):
        @pl.when(core == SUMMING)
        def _():
            whole_of(far.at[p, s], far_send.at[0], far_recv.at[p, s]).wait_recv()
            coefs[p, s, part_of(my_quarter)] = (near_sum[p, s] + far[p, s, 1]) + (far[p, s, 0] + far[p, s, 2])
            for by in (2, 1, 3):
                spread_copy(p, s, by, 1 - SUMMING).start()
                spread_copy(p, s, by, SUMMING).start()
            spread_copy(p, s, 0, 1 - SUMMING).start()

    def update(p, s):
        @pl.when(core == SUMMING)
        def _():
            whole_of(near.at[p, s, pl.ds(0, 3)], spread_send.at[0], spread_recv.at[p, s]).wait_recv()

        @pl.when(core != SUMMING)
        def _():
            whole_of(near.at[p, s, pl.ds(0, 4)], spread_send.at[0], spread_recv.at[p, s]).wait_recv()

        scaled = product(coefs[p, s], t_high[p], t_low[p], 0)
        x_turned[columns(s), :] = x_turned[columns(s), :] - product(scaled, w_high[p], w_low[p], 0)

    with scope("g0"):
        gather_0(last)
        announce(0)
        load_x = pltpu.make_async_copy(x_ref, x_in, load_sem.at[2 * panels])
        load_x.start()
        later_loads = [copy for p in range(last - 1, -1, -1) for copy in load(p)]
        load_x.wait()
        x_turned[...] = x_in[...].T
    with scope("g1"):
        gather_1(last)
        heard(0)
        announce(1)
    with scope("g2"):
        gather_2(last)
        heard(1)
        announce(2)
    with scope("g3"):
        gather_3(last)
        for copy in later_loads:
            copy.wait()
        gather_0(last - 1)
    with scope("g4"):
        gather_4(last)
        heard(2)
    with scope("prep"):
        split_panel(last)
    for s in range(STREAMS):
        with scope("project"):
            project(last, s)
    with scope("g1n"):
        gather_1(last - 1)
    for p in range(last, -1, -1):
        if p == 0:
            with scope("alone"):
                alone_wait().wait_recv()
                factor_copy(ALONE).start()
        with scope("turn"):
            turn_panel(p)
        for s in range(STREAMS):
            with scope(f"near{s}"):
                sum_near(p, s)
        if p > 0:
            with scope("g2n"):
                gather_2(p - 1)
            with scope("g3n"):
                gather_3(p - 1)
                if p > 1:
                    gather_0(p - 2)
                else:
                    send_alone()
        for s in range(STREAMS):
            with scope(f"far{s}"):
                sum_far(p, s)
        if p > 0:
            with scope("g4n"):
                gather_4(p - 1)
                factor_copy(CARRIED[p - 1]).start()
            with scope("prepn"):
                split_panel(p - 1)
        if p > 1:
            with scope("g1n"):
                gather_1(p - 2)
        with scope("factor"):
            split_factor(p)
        for s in range(STREAMS):
            with scope(f"update{s}"):
                update(p, s)
            if p > 0:
                with scope("project"):
                    project(p - 1, s)
    with scope("out"):
        out_ref[...] = x_turned[...].T
    with scope("drain"):
        for p in range(panels):
            whole = blocks.at[p, pl.ds(0, 15), pl.ds(0, length_of(p)), :]
            pltpu.make_async_remote_copy(
                src_ref=whole, dst_ref=whole, send_sem=gather_send.at[p], recv_sem=gather_last.at[p],
                device_id={"core": 1 - core}, device_id_type=MESH,
            ).wait_send()
        to_core(other_t, other_t, 0, factor_recv.at[0]).wait_send()
        alone_wait().wait_send()
        @pl.when(core == SUMMING)
        def _():
            whole_of(near.at[:, :, pl.ds(0, 3)], near_send.at[0], near_recv.at[0, 0]).wait_send()
            whole_of(far, far_send.at[0], far_recv.at[0, 0]).wait_send()
            whole_of(near.at[:, :, pl.ds(0, 7)], spread_send.at[0], spread_recv.at[0, 0]).wait_send()

        @pl.when(core != SUMMING)
        def _():
            whole_of(near.at[:, :, pl.ds(0, 4)], near_send.at[0], near_recv.at[0, 0]).wait_send()


def per_device(vectors, reflectors, triangles):
    panels, rows, width = reflectors.shape
    length, count = vectors.shape
    turned = jnp.swapaxes(triangles, 1, 2)
    half = turned.shape[1] // 2
    part = count // STREAMS // 4
    f32, bf16 = jnp.float32, jnp.bfloat16
    dma = pltpu.SemaphoreType.DMA
    return pl.pallas_call(
        kernel,
        out_shape=jax.ShapeDtypeStruct(vectors.shape, f32),
        in_specs=[pl.BlockSpec(memory_space=pltpu.HBM)] * 3,
        out_specs=pl.BlockSpec(memory_space=pltpu.VMEM),
        scratch_shapes=[
            pltpu.VMEM((length, count), f32),
            pltpu.VMEM((count, length), f32),
            pltpu.VMEM((panels, 16, rows + half, width), f32),
            pltpu.VMEM((16, half, width), f32),
            pltpu.VMEM((panels, 16, half, width), f32),
            pltpu.VMEM((panels, 16 * rows, width), bf16),
            pltpu.VMEM((panels, 16 * rows, width), bf16),
            pltpu.VMEM((panels, width, 16 * rows), bf16),
            pltpu.VMEM((panels, width, 16 * rows), bf16),
            pltpu.VMEM((panels, width, width), bf16),
            pltpu.VMEM((panels, width, width), bf16),
            pltpu.VMEM((panels, STREAMS, 4 * part, width), f32),
            pltpu.VMEM((panels, STREAMS, 8, part, width), f32),
            pltpu.VMEM((panels, STREAMS, part, width), f32),
            pltpu.VMEM((panels, STREAMS, 3, part, width), f32),
            pltpu.VMEM((panels, STREAMS, 4 * part, width), f32),
            dma((2 * panels + 1,)), pltpu.SemaphoreType.REGULAR((3,)),
            dma((panels,)), dma((panels, 4)), dma((panels, 2)), dma((panels, 16)), dma((panels,)),
            dma((1,)), dma((1,)), dma((1,)), dma((panels,)), dma((1,)), dma((panels, STREAMS)),
            dma((1,)), dma((panels, STREAMS)), dma((1,)), dma((panels, STREAMS)),
        ],
        compiler_params=pltpu.CompilerParams(collective_id=0, has_side_effects=True, vmem_limit_bytes=36 * 2**20),
    )(*(pltpu.with_memory_space_constraint(a, pltpu.HBM) for a in (vectors, reflectors, turned)))


def solution(mesh):
    finer = Mesh(mesh.devices.reshape(16, 2, 4, 4), ("z", "core", "y", "x"))
    placed = (P(ROW, VEC), P(None, ROW + VEC, None), P(None, None, VEC))
    return jax.shard_map(
        per_device, mesh=finer, in_specs=placed, out_specs=P(ROW, VEC), check_vma=False
    )
```

```python
import functools

import jax
import jax.numpy as jnp
from jax import lax
from jax.experimental import pallas as pl
from jax.experimental.pallas import tpu as pltpu
from jax.sharding import Mesh
from jax.sharding import PartitionSpec as P

MESH = pl.DeviceIdType.MESH
VEC = ("y", "x")
ROW = ("z", "core")
STREAMS = 2
SUMMING = 1

CARRIED = (1, 2, None)
ALONE = 0
OFFSETS = (0, -1, 1, 2)


def halves(value):
    high = value.astype(jnp.bfloat16)
    low = (value - high.astype(jnp.float32)).astype(jnp.bfloat16)
    return high, low


def product(a, b_high, b_low, contracted):
    a_high, a_low = halves(a)
    count = a.shape[0]
    dot = functools.partial(
        lax.dot_general, dimension_numbers=(((1,), (contracted,)), ((), ())), preferred_element_type=jnp.float32
    )
    both = dot(jnp.concatenate([a_high, a_low], axis=0), b_high)
    return both[:count] + (dot(a_high, b_low) + both[count:])


def kernel(
    x_ref, reflectors_ref, factors_ref, out_ref,
    x_in, x_turned, blocks, alone, other_t, v_high, v_low, w_high, w_low, t_high, t_low, partial_c, near, near_sum, far, coefs,
    load_sem, entered, gather_send, gather_first, gather_opposite, gather_second, gather_last,
    alone_send, alone_recv, core_send, factor_recv, near_send, near_recv, far_send, far_recv, spread_send, spread_recv,
):
    panels, rows, width = reflectors_ref.shape
    half_t = factors_ref.shape[1] // 2
    z, core = lax.axis_index("z"), lax.axis_index("core")
    y, x = lax.axis_index("y"), lax.axis_index("x")
    depth = lax.axis_size("z")
    place = {"x": x, "y": y}
    me = y * 4 + x
    last = panels - 1

    def length_of(p):
        return rows + half_t * (CARRIED[p] is not None)

    def scope(name):
        return jax.named_scope(name)

    def step(axis, by):
        return lax.rem(place[axis] + by + 4, 4)

    def up(by):
        return lax.rem(z + by + depth, depth)

    def own_factor(q, there):
        mine = pl.ds(pl.multiple_of(core * half_t, half_t), half_t)
        return pltpu.make_async_copy(factors_ref.at[q, mine, :], there, load_sem.at[2 * q + 1])

    def load(p):
        copies = [pltpu.make_async_copy(reflectors_ref.at[p], blocks.at[p, me, pl.ds(0, rows), :], load_sem.at[2 * p])]
        if CARRIED[p] is not None:
            copies.append(own_factor(CARRIED[p], blocks.at[p, me, pl.ds(rows, half_t), :]))
        if p == 0:
            copies.append(own_factor(ALONE, alone.at[me]))
        for copy in copies:
            copy.start()
        return copies

    first_load = load(last)
    with scope("barrier"):
        barrier = pltpu.get_barrier_semaphore()
        for axis in ("x", "y"):
            for by in (1, -1, 2):
                pl.semaphore_signal(barrier, inc=1, device_id={axis: step(axis, by)}, device_id_type=MESH)
        for by in (1, -1):
            for other in (core, 1 - core):
                pl.semaphore_signal(barrier, inc=1, device_id={"z": up(by), "core": other}, device_id_type=MESH)
        pl.semaphore_signal(barrier, inc=1, device_id={"core": 1 - core}, device_id_type=MESH)
        for copy in first_load:
            copy.wait()
        pl.semaphore_wait(barrier, 11)

    def announce(round_):
        for by in (1, -1):
            to = up(by * (1, 2, 4)[round_])
            pl.semaphore_signal(entered.at[round_], inc=1, device_id={"z": to}, device_id_type=MESH)
            if round_ == 0:
                pl.semaphore_signal(entered.at[0], inc=1, device_id={"z": to, "core": 1 - core}, device_id_type=MESH)

    def heard(round_):
        pl.semaphore_wait(entered.at[round_], 4 if round_ == 0 else 2)

    def block_at(half, first, second):
        first_axis, second_axis = ("x", "y") if half == 0 else ("y", "x")
        at = {first_axis: step(first_axis, first), second_axis: step(second_axis, second)}
        return at["y"] * 4 + at["x"]

    def transfer(panel, half, recv, part, first, second, second_leg, by):
        size = length_of(panel) // 2
        start, cut = half * size, (size // 2 + 7 * (1 - half)) // 8 * 8
        start, size = {"all": (start, size), "plus": (start, cut), "minus": (start + cut, size - cut)}[part]
        there = blocks.at[panel, block_at(half, first, second), pl.ds(start, size), :]
        axis = ("x", "y")[(half + second_leg) % 2]
        return pltpu.make_async_remote_copy(
            src_ref=there, dst_ref=there, send_sem=gather_send.at[panel], recv_sem=recv,
            device_id={axis: step(axis, by)}, device_id_type=MESH,
        )

    def side(by):
        return 0 if by == 1 else 1

    def first_leg(p, h, by, first=0):
        return transfer(p, h, gather_first.at[p, 2 * h + side(by)], "all", first, 0, 0, by)

    def opposite(p, h, part, by, first):
        return transfer(p, h, gather_opposite.at[p, h], part, first, 0, 0, by)

    def straight(p, h):
        return transfer(p, h, gather_opposite.at[p, h], "all", 0, 0, 0, 2)

    def second_leg(p, h, s, by, second=0):
        return transfer(p, h, gather_second.at[p, (h * 4 + s) * 2 + side(by)], "all", OFFSETS[s], second, 1, by)

    def final_leg(p, h, s, part, by):
        return transfer(p, h, gather_last.at[p], part, OFFSETS[s], -by, 1, by)

    def gather_0(p):
        for h in (0, 1):
            for by in (1, -1):
                first_leg(p, h, by).start()

        @pl.when(core != SUMMING)
        def _():
            for h in (0, 1):
                straight(p, h).start()

        for h in (0, 1):
            for by in (1, -1):
                second_leg(p, h, 0, by).start()

    def gather_1(p):
        for h in (0, 1):
            first_leg(p, h, 1, -1).wait_recv()
            first_leg(p, h, -1, 1).wait_recv()

            @pl.when(core == SUMMING)
            def _():
                opposite(p, h, "plus", 1, -1).start()
                opposite(p, h, "minus", -1, 1).start()

        for h in (0, 1):
            for s in (1, 2):
                for by in (1, -1):
                    second_leg(p, h, s, by).start()

    def gather_2(p):
        for h in (0, 1):
            opposite(p, h, "all", 1, 2).wait_recv()
            for by in (1, -1):
                second_leg(p, h, 3, by).start()

    def gather_3(p):
        for s in range(4):
            for h in (0, 1):
                for by, part in ((1, "plus"), (-1, "minus")):
                    second_leg(p, h, s, by, -by).wait_recv()
                    final_leg(p, h, s, part, by).start()

    def gather_4(p):
        whole = blocks.at[p, pl.ds(0, 4), pl.ds(0, length_of(p)), :]
        pltpu.make_async_remote_copy(
            src_ref=whole, dst_ref=whole, send_sem=gather_send.at[p], recv_sem=gather_last.at[p],
            device_id={"core": 1 - core}, device_id_type=MESH,
        ).wait_recv()

    def to_core(src, dst, send, recv):
        return pltpu.make_async_remote_copy(
            src_ref=src, dst_ref=dst, send_sem=core_send.at[send], recv_sem=recv,
            device_id={"core": 1 - core}, device_id_type=MESH,
        )

    def factor_copy(q):
        here = alone if q == ALONE else blocks.at[CARRIED.index(q), :, pl.ds(rows, half_t), :]
        return to_core(here, other_t.at[q], 0, factor_recv.at[q])

    def factor_rows(b, core_):
        return pl.ds(pl.multiple_of(b * 32 + core_ * 16, 16), 16)

    def split_panel(p):
        @pl.loop(0, 16)
        def _(b):
            at = pl.ds(pl.multiple_of(b * rows, rows), rows)
            v_high[p, at, :], v_low[p, at, :] = halves(blocks[p, b, 0:rows, :])

    def turn_panel(p):
        @pl.loop(0, 8)
        def _(i):
            at = pl.ds(pl.multiple_of(i * 2 * rows, 2 * rows), 2 * rows)
            two = jnp.concatenate([blocks[p, 2 * i, 0:rows, :], blocks[p, 2 * i + 1, 0:rows, :]], axis=0)
            w_high[p, :, at], w_low[p, :, at] = halves(two.T)

    def split_factor(q):
        @pl.loop(0, 16)
        def _(b):
            mine = alone[b] if q == ALONE else blocks[CARRIED.index(q), b, rows : rows + half_t, :]
            t_high[q, factor_rows(b, core), :], t_low[q, factor_rows(b, core), :] = halves(mine)

        factor_copy(q).wait_recv()

        @pl.loop(0, 16)
        def _(b):
            t_high[q, factor_rows(b, 1 - core), :], t_low[q, factor_rows(b, 1 - core), :] = halves(other_t[q, b])

    def send_alone():
        for dy in range(4):
            for dx in range(4):
                if dy or dx:
                    pltpu.make_async_remote_copy(
                        src_ref=alone.at[me], dst_ref=alone.at[me], send_sem=alone_send.at[0], recv_sem=alone_recv.at[0],
                        device_id={"y": step("y", dy), "x": step("x", dx)}, device_id_type=MESH,
                    ).start()

    def alone_wait():
        others = alone.at[pl.ds(0, 15)]
        return pltpu.make_async_remote_copy(
            src_ref=others, dst_ref=others, send_sem=alone_send.at[0], recv_sem=alone_recv.at[0],
            device_id={"core": 1 - core}, device_id_type=MESH,
        )

    count = x_turned.shape[0] // STREAMS
    part = count // 4

    def first_of(quarter):
        return quarter % 2 * 2 + quarter // 2 * 8

    def chip_at(quarter, group, member):
        return lax.rem(first_of(quarter) + group * 4 + member, depth)

    def summing(group):
        return 1 + group // 2

    def group_of(quarter):
        return lax.rem(z - first_of(quarter) + depth, depth) // 4

    my_quarter = lax.rem(z + 3, 4) // 2 + lax.rem(z + 6 * (1 - lax.rem(z, 2)), depth) // 8 * 2
    my_group = group_of(my_quarter)
    my_member = summing(my_group)

    def part_of(quarter):
        return pl.ds(pl.multiple_of(quarter * part, part), part)

    def near_copy(p, s, by):
        quarter = lax.rem(my_quarter + by, 4)
        group = group_of(quarter)
        member = lax.rem(z - first_of(quarter) + depth, 4)
        return pltpu.make_async_remote_copy(
            src_ref=partial_c.at[p, s, part_of(quarter)], dst_ref=near.at[p, s, member * 2 + core],
            send_sem=near_send.at[0], recv_sem=near_recv.at[p, s],
            device_id={"z": chip_at(quarter, group, summing(group)), "core": SUMMING}, device_id_type=MESH,
        )

    def far_copy(p, s, by):
        group = lax.rem(my_group + by, 4)
        return pltpu.make_async_remote_copy(
            src_ref=near_sum.at[p, s], dst_ref=far.at[p, s, by - 1],
            send_sem=far_send.at[0], recv_sem=far_recv.at[p, s],
            device_id={"z": chip_at(my_quarter, group, summing(group)), "core": SUMMING}, device_id_type=MESH,
        )

    def spread_copy(p, s, by, other):
        own = coefs.at[p, s, part_of(my_quarter)]
        return pltpu.make_async_remote_copy(
            src_ref=own, dst_ref=own, send_sem=spread_send.at[0], recv_sem=spread_recv.at[p, s],
            device_id={"z": chip_at(my_quarter, my_group, lax.rem(my_member + by, 4)), "core": other},
            device_id_type=MESH,
        )

    def whole_of(ref, send, recv):
        return pltpu.make_async_remote_copy(
            src_ref=ref, dst_ref=ref, send_sem=send, recv_sem=recv, device_id={"core": 1 - core}, device_id_type=MESH
        )

    def columns(s):
        return slice(s * count, (s + 1) * count)

    def project(p, s):
        partial_c[p, s] = product(x_turned[columns(s), :], v_high[p], v_low[p], 0)
        for by in (2, 1, 3):
            near_copy(p, s, by).start()

        @pl.when(core != SUMMING)
        def _():
            near_copy(p, s, 0).start()

    def sum_near(p, s):
        @pl.when(core == SUMMING)
        def _():
            near[p, s, my_member * 2 + SUMMING] = partial_c[p, s, part_of(my_quarter)]
            whole_of(near.at[p, s, pl.ds(0, 7)], near_send.at[0], near_recv.at[p, s]).wait_recv()
            pairs = [near[p, s, i] + near[p, s, i + 1] for i in range(0, 8, 2)]
            near_sum[p, s] = (pairs[0] + pairs[1]) + (pairs[2] + pairs[3])
            for by in (2, 1, 3):
                far_copy(p, s, by).start()

    def sum_far(p, s):
        @pl.when(core == SUMMING)
        def _():
            whole_of(far.at[p, s], far_send.at[0], far_recv.at[p, s]).wait_recv()
            coefs[p, s, part_of(my_quarter)] = (near_sum[p, s] + far[p, s, 1]) + (far[p, s, 0] + far[p, s, 2])
            for by in (2, 1, 3):
                spread_copy(p, s, by, 1 - SUMMING).start()
                spread_copy(p, s, by, SUMMING).start()
            spread_copy(p, s, 0, 1 - SUMMING).start()

    def update(p, s):
        @pl.when(core == SUMMING)
        def _():
            whole_of(near.at[p, s, pl.ds(0, 3)], spread_send.at[0], spread_recv.at[p, s]).wait_recv()

        @pl.when(core != SUMMING)
        def _():
            whole_of(near.at[p, s, pl.ds(0, 4)], spread_send.at[0], spread_recv.at[p, s]).wait_recv()

        scaled = product(coefs[p, s], t_high[p], t_low[p], 0)
        x_turned[columns(s), :] = x_turned[columns(s), :] - product(scaled, w_high[p], w_low[p], 0)

    with scope("g0"):
        gather_0(last)
        announce(0)
        load_x = pltpu.make_async_copy(x_ref, x_in, load_sem.at[2 * panels])
        load_x.start()
        later_loads = [copy for p in range(last - 1, -1, -1) for copy in load(p)]
        load_x.wait()
        x_turned[...] = x_in[...].T
    with scope("g1"):
        gather_1(last)
        heard(0)
        announce(1)
    with scope("g2"):
        gather_2(last)
        heard(1)
        announce(2)
    with scope("g3"):
        gather_3(last)
        for copy in later_loads:
            copy.wait()
        gather_0(last - 1)
    with scope("g4"):
        gather_4(last)
        heard(2)
    with scope("prep"):
        split_panel(last)
    for s in range(STREAMS):
        with scope("project"):
            project(last, s)
    with scope("g1n"):
        gather_1(last - 1)
    for p in range(last, -1, -1):
        if p == 0:
            with scope("alone"):
                alone_wait().wait_recv()
                factor_copy(ALONE).start()
        with scope("turn"):
            turn_panel(p)
        if p == 1:
            with scope("g2n"):
                gather_2(p - 1)
        for s in range(STREAMS):
            with scope(f"near{s}"):
                sum_near(p, s)
        if p > 0:
            if p > 1:
                with scope("g2n"):
                    gather_2(p - 1)
            with scope("g3n"):
                gather_3(p - 1)
                if p > 1:
                    gather_0(p - 2)
                else:
                    send_alone()
        for s in range(STREAMS):
            with scope(f"far{s}"):
                sum_far(p, s)
        if p > 0:
            with scope("g4n"):
                gather_4(p - 1)
                factor_copy(CARRIED[p - 1]).start()
            with scope("prepn"):
                split_panel(p - 1)
        if p > 1:
            with scope("g1n"):
                gather_1(p - 2)
        with scope("factor"):
            split_factor(p)
        for s in range(STREAMS):
            with scope(f"update{s}"):
                update(p, s)
            if p > 0:
                with scope("project"):
                    project(p - 1, s)
    with scope("out"):
        out_ref[...] = x_turned[...].T
    with scope("drain"):
        for p in range(panels):
            whole = blocks.at[p, pl.ds(0, 15), pl.ds(0, length_of(p)), :]
            pltpu.make_async_remote_copy(
                src_ref=whole, dst_ref=whole, send_sem=gather_send.at[p], recv_sem=gather_last.at[p],
                device_id={"core": 1 - core}, device_id_type=MESH,
            ).wait_send()
        to_core(other_t, other_t, 0, factor_recv.at[0]).wait_send()
        alone_wait().wait_send()
        @pl.when(core == SUMMING)
        def _():
            whole_of(near.at[:, :, pl.ds(0, 3)], near_send.at[0], near_recv.at[0, 0]).wait_send()
            whole_of(far, far_send.at[0], far_recv.at[0, 0]).wait_send()
            whole_of(near.at[:, :, pl.ds(0, 7)], spread_send.at[0], spread_recv.at[0, 0]).wait_send()

        @pl.when(core != SUMMING)
        def _():
            whole_of(near.at[:, :, pl.ds(0, 4)], near_send.at[0], near_recv.at[0, 0]).wait_send()


def per_device(vectors, reflectors, triangles):
    panels, rows, width = reflectors.shape
    length, count = vectors.shape
    turned = jnp.swapaxes(triangles, 1, 2)
    half = turned.shape[1] // 2
    part = count // STREAMS // 4
    f32, bf16 = jnp.float32, jnp.bfloat16
    dma = pltpu.SemaphoreType.DMA
    return pl.pallas_call(
        kernel,
        out_shape=jax.ShapeDtypeStruct(vectors.shape, f32),
        in_specs=[pl.BlockSpec(memory_space=pltpu.HBM)] * 3,
        out_specs=pl.BlockSpec(memory_space=pltpu.VMEM),
        scratch_shapes=[
            pltpu.VMEM((length, count), f32),
            pltpu.VMEM((count, length), f32),
            pltpu.VMEM((panels, 16, rows + half, width), f32),
            pltpu.VMEM((16, half, width), f32),
            pltpu.VMEM((panels, 16, half, width), f32),
            pltpu.VMEM((panels, 16 * rows, width), bf16),
            pltpu.VMEM((panels, 16 * rows, width), bf16),
            pltpu.VMEM((panels, width, 16 * rows), bf16),
            pltpu.VMEM((panels, width, 16 * rows), bf16),
            pltpu.VMEM((panels, width, width), bf16),
            pltpu.VMEM((panels, width, width), bf16),
            pltpu.VMEM((panels, STREAMS, 4 * part, width), f32),
            pltpu.VMEM((panels, STREAMS, 8, part, width), f32),
            pltpu.VMEM((panels, STREAMS, part, width), f32),
            pltpu.VMEM((panels, STREAMS, 3, part, width), f32),
            pltpu.VMEM((panels, STREAMS, 4 * part, width), f32),
            dma((2 * panels + 1,)), pltpu.SemaphoreType.REGULAR((3,)),
            dma((panels,)), dma((panels, 4)), dma((panels, 2)), dma((panels, 16)), dma((panels,)),
            dma((1,)), dma((1,)), dma((1,)), dma((panels,)), dma((1,)), dma((panels, STREAMS)),
            dma((1,)), dma((panels, STREAMS)), dma((1,)), dma((panels, STREAMS)),
        ],
        compiler_params=pltpu.CompilerParams(collective_id=0, has_side_effects=True, vmem_limit_bytes=36 * 2**20),
    )(*(pltpu.with_memory_space_constraint(a, pltpu.HBM) for a in (vectors, reflectors, turned)))


def solution(mesh):
    finer = Mesh(mesh.devices.reshape(16, 2, 4, 4), ("z", "core", "y", "x"))
    placed = (P(ROW, VEC), P(None, ROW + VEC, None), P(None, None, VEC))
    return jax.shard_map(
        per_device, mesh=finer, in_specs=placed, out_specs=P(ROW, VEC), check_vma=False
    )
```

```python
import functools

import jax
import jax.numpy as jnp
from jax import lax
from jax.experimental import pallas as pl
from jax.experimental.pallas import tpu as pltpu
from jax.sharding import Mesh
from jax.sharding import PartitionSpec as P

MESH = pl.DeviceIdType.MESH
VEC = ("y", "x")
ROW = ("z", "core")
STREAMS = 2
SUMMING = 1

CARRIED = (1, 2, None)
ALONE = 0
OFFSETS = (0, -1, 1, 2)


def halves(value):
    high = value.astype(jnp.bfloat16)
    low = (value - high.astype(jnp.float32)).astype(jnp.bfloat16)
    return high, low


def product(a, b_high, b_low, contracted):
    a_high, a_low = halves(a)
    count = a.shape[0]
    dot = functools.partial(
        lax.dot_general, dimension_numbers=(((1,), (contracted,)), ((), ())), preferred_element_type=jnp.float32
    )
    both = dot(jnp.concatenate([a_high, a_low], axis=0), b_high)
    return both[:count] + (dot(a_high, b_low) + both[count:])


def kernel(
    x_ref, reflectors_ref, factors_ref, out_ref,
    x_in, x_turned, blocks, alone, other_t, v_high, v_low, w_high, w_low, t_high, t_low, partial_c, near, near_sum, far, coefs,
    load_sem, entered, gather_send, gather_first, gather_opposite, gather_second, gather_last,
    alone_send, alone_recv, core_send, factor_recv, near_send, near_recv, far_send, far_recv, spread_send, spread_recv,
):
    panels, rows, width = reflectors_ref.shape
    half_t = factors_ref.shape[1] // 2
    z, core = lax.axis_index("z"), lax.axis_index("core")
    y, x = lax.axis_index("y"), lax.axis_index("x")
    depth = lax.axis_size("z")
    place = {"x": x, "y": y}
    me = y * 4 + x
    last = panels - 1

    def length_of(p):
        return rows + half_t * (CARRIED[p] is not None)

    def scope(name):
        return jax.named_scope(name)

    def step(axis, by):
        return lax.rem(place[axis] + by + 4, 4)

    def up(by):
        return lax.rem(z + by + depth, depth)

    def own_factor(q, there):
        mine = pl.ds(pl.multiple_of(core * half_t, half_t), half_t)
        return pltpu.make_async_copy(factors_ref.at[q, mine, :], there, load_sem.at[2 * q + 1])

    def load(p):
        copies = [pltpu.make_async_copy(reflectors_ref.at[p], blocks.at[p, me, pl.ds(0, rows), :], load_sem.at[2 * p])]
        if CARRIED[p] is not None:
            copies.append(own_factor(CARRIED[p], blocks.at[p, me, pl.ds(rows, half_t), :]))
        if p == 0:
            copies.append(own_factor(ALONE, alone.at[me]))
        for copy in copies:
            copy.start()
        return copies

    first_load = load(last)
    with scope("barrier"):
        barrier = pltpu.get_barrier_semaphore()
        for axis in ("x", "y"):
            for by in (1, -1, 2):
                pl.semaphore_signal(barrier, inc=1, device_id={axis: step(axis, by)}, device_id_type=MESH)
        for by in (1, -1):
            for other in (core, 1 - core):
                pl.semaphore_signal(barrier, inc=1, device_id={"z": up(by), "core": other}, device_id_type=MESH)
        pl.semaphore_signal(barrier, inc=1, device_id={"core": 1 - core}, device_id_type=MESH)
        for copy in first_load:
            copy.wait()
        pl.semaphore_wait(barrier, 11)

    def announce(round_):
        for by in (1, -1):
            to = up(by * (1, 2, 4)[round_])
            pl.semaphore_signal(entered.at[round_], inc=1, device_id={"z": to}, device_id_type=MESH)
            if round_ == 0:
                pl.semaphore_signal(entered.at[0], inc=1, device_id={"z": to, "core": 1 - core}, device_id_type=MESH)

    def heard(round_):
        pl.semaphore_wait(entered.at[round_], 4 if round_ == 0 else 2)

    def block_at(half, first, second):
        first_axis, second_axis = ("x", "y") if half == 0 else ("y", "x")
        at = {first_axis: step(first_axis, first), second_axis: step(second_axis, second)}
        return at["y"] * 4 + at["x"]

    def transfer(panel, half, recv, part, first, second, second_leg, by):
        size = length_of(panel) // 2
        start, cut = half * size, (size // 2 + 7 * (1 - half)) // 8 * 8
        start, size = {"all": (start, size), "plus": (start, cut), "minus": (start + cut, size - cut)}[part]
        there = blocks.at[panel, block_at(half, first, second), pl.ds(start, size), :]
        axis = ("x", "y")[(half + second_leg) % 2]
        return pltpu.make_async_remote_copy(
            src_ref=there, dst_ref=there, send_sem=gather_send.at[panel], recv_sem=recv,
            device_id={axis: step(axis, by)}, device_id_type=MESH,
        )

    def side(by):
        return 0 if by == 1 else 1

    def first_leg(p, h, by, first=0):
        return transfer(p, h, gather_first.at[p, 2 * h + side(by)], "all", first, 0, 0, by)

    def opposite(p, h, part, by, first):
        return transfer(p, h, gather_opposite.at[p, h], part, first, 0, 0, by)

    def straight(p, h):
        return transfer(p, h, gather_opposite.at[p, h], "all", 0, 0, 0, 2)

    def second_leg(p, h, s, by, second=0):
        return transfer(p, h, gather_second.at[p, (h * 4 + s) * 2 + side(by)], "all", OFFSETS[s], second, 1, by)

    def final_leg(p, h, s, part, by):
        return transfer(p, h, gather_last.at[p], part, OFFSETS[s], -by, 1, by)

    def gather_0(p):
        for h in (0, 1):
            for by in (1, -1):
                first_leg(p, h, by).start()

        @pl.when(core != SUMMING)
        def _():
            for h in (0, 1):
                straight(p, h).start()

        for h in (0, 1):
            for by in (1, -1):
                second_leg(p, h, 0, by).start()

    def gather_1(p):
        for h in (0, 1):
            first_leg(p, h, 1, -1).wait_recv()
            first_leg(p, h, -1, 1).wait_recv()

            @pl.when(core == SUMMING)
            def _():
                opposite(p, h, "plus", 1, -1).start()
                opposite(p, h, "minus", -1, 1).start()

        for h in (0, 1):
            for s in (1, 2):
                for by in (1, -1):
                    second_leg(p, h, s, by).start()

    def gather_2(p):
        for h in (0, 1):
            opposite(p, h, "all", 1, 2).wait_recv()
            for by in (1, -1):
                second_leg(p, h, 3, by).start()

    def gather_3(p):
        for s in range(4):
            for h in (0, 1):
                for by, part in ((1, "plus"), (-1, "minus")):
                    second_leg(p, h, s, by, -by).wait_recv()
                    final_leg(p, h, s, part, by).start()

    def gather_4(p):
        whole = blocks.at[p, pl.ds(0, 4), pl.ds(0, length_of(p)), :]
        pltpu.make_async_remote_copy(
            src_ref=whole, dst_ref=whole, send_sem=gather_send.at[p], recv_sem=gather_last.at[p],
            device_id={"core": 1 - core}, device_id_type=MESH,
        ).wait_recv()

    def to_core(src, dst, send, recv):
        return pltpu.make_async_remote_copy(
            src_ref=src, dst_ref=dst, send_sem=core_send.at[send], recv_sem=recv,
            device_id={"core": 1 - core}, device_id_type=MESH,
        )

    def factor_copy(q):
        here = alone if q == ALONE else blocks.at[CARRIED.index(q), :, pl.ds(rows, half_t), :]
        return to_core(here, other_t.at[q], 0, factor_recv.at[q])

    def factor_rows(b, core_):
        return pl.ds(pl.multiple_of(b * 32 + core_ * 16, 16), 16)

    def split_panel(p):
        @pl.loop(0, 16)
        def _(b):
            at = pl.ds(pl.multiple_of(b * rows, rows), rows)
            v_high[p, at, :], v_low[p, at, :] = halves(blocks[p, b, 0:rows, :])

    def turn_panel(p):
        @pl.loop(0, 8)
        def _(i):
            at = pl.ds(pl.multiple_of(i * 2 * rows, 2 * rows), 2 * rows)
            two = jnp.concatenate([blocks[p, 2 * i, 0:rows, :], blocks[p, 2 * i + 1, 0:rows, :]], axis=0)
            w_high[p, :, at], w_low[p, :, at] = halves(two.T)

    def split_factor(q):
        @pl.loop(0, 16)
        def _(b):
            mine = alone[b] if q == ALONE else blocks[CARRIED.index(q), b, rows : rows + half_t, :]
            t_high[q, factor_rows(b, core), :], t_low[q, factor_rows(b, core), :] = halves(mine)

        factor_copy(q).wait_recv()

        @pl.loop(0, 16)
        def _(b):
            t_high[q, factor_rows(b, 1 - core), :], t_low[q, factor_rows(b, 1 - core), :] = halves(other_t[q, b])

    def send_alone():
        for dy in range(4):
            for dx in range(4):
                if dy or dx:
                    pltpu.make_async_remote_copy(
                        src_ref=alone.at[me], dst_ref=alone.at[me], send_sem=alone_send.at[0], recv_sem=alone_recv.at[0],
                        device_id={"y": step("y", dy), "x": step("x", dx)}, device_id_type=MESH,
                    ).start()

    def alone_wait():
        others = alone.at[pl.ds(0, 15)]
        return pltpu.make_async_remote_copy(
            src_ref=others, dst_ref=others, send_sem=alone_send.at[0], recv_sem=alone_recv.at[0],
            device_id={"core": 1 - core}, device_id_type=MESH,
        )

    count = x_turned.shape[0] // STREAMS
    part = count // 4

    def first_of(quarter):
        return quarter % 2 * 2 + quarter // 2 * 8

    def chip_at(quarter, group, member):
        return lax.rem(first_of(quarter) + group * 4 + member, depth)

    def summing(group):
        return 1 + group // 2

    def group_of(quarter):
        return lax.rem(z - first_of(quarter) + depth, depth) // 4

    my_quarter = lax.rem(z + 3, 4) // 2 + lax.rem(z + 6 * (1 - lax.rem(z, 2)), depth) // 8 * 2
    my_group = group_of(my_quarter)
    my_member = summing(my_group)

    def part_of(quarter):
        return pl.ds(pl.multiple_of(quarter * part, part), part)

    def near_copy(p, s, by):
        quarter = lax.rem(my_quarter + by, 4)
        group = group_of(quarter)
        member = lax.rem(z - first_of(quarter) + depth, 4)
        return pltpu.make_async_remote_copy(
            src_ref=partial_c.at[p, s, part_of(quarter)], dst_ref=near.at[p, s, member * 2 + core],
            send_sem=near_send.at[0], recv_sem=near_recv.at[p, s],
            device_id={"z": chip_at(quarter, group, summing(group)), "core": SUMMING}, device_id_type=MESH,
        )

    def far_copy(p, s, by):
        group = lax.rem(my_group + by, 4)
        return pltpu.make_async_remote_copy(
            src_ref=near_sum.at[p, s], dst_ref=far.at[p, s, by - 1],
            send_sem=far_send.at[0], recv_sem=far_recv.at[p, s],
            device_id={"z": chip_at(my_quarter, group, summing(group)), "core": SUMMING}, device_id_type=MESH,
        )

    def spread_copy(p, s, by, other):
        own = coefs.at[p, s, part_of(my_quarter)]
        return pltpu.make_async_remote_copy(
            src_ref=own, dst_ref=own, send_sem=spread_send.at[0], recv_sem=spread_recv.at[p, s],
            device_id={"z": chip_at(my_quarter, my_group, lax.rem(my_member + by, 4)), "core": other},
            device_id_type=MESH,
        )

    def whole_of(ref, send, recv):
        return pltpu.make_async_remote_copy(
            src_ref=ref, dst_ref=ref, send_sem=send, recv_sem=recv, device_id={"core": 1 - core}, device_id_type=MESH
        )

    def columns(s):
        return slice(s * count, (s + 1) * count)

    def project(p, s):
        partial_c[p, s] = product(x_turned[columns(s), :], v_high[p], v_low[p], 0)
        for by in (2, 1, 3):
            near_copy(p, s, by).start()

        @pl.when(core != SUMMING)
        def _():
            near_copy(p, s, 0).start()

    def sum_near(p, s):
        @pl.when(core == SUMMING)
        def _():
            near[p, s, my_member * 2 + SUMMING] = partial_c[p, s, part_of(my_quarter)]
            whole_of(near.at[p, s, pl.ds(0, 7)], near_send.at[0], near_recv.at[p, s]).wait_recv()
            pairs = [near[p, s, i] + near[p, s, i + 1] for i in range(0, 8, 2)]
            near_sum[p, s] = (pairs[0] + pairs[1]) + (pairs[2] + pairs[3])
            for by in (2, 1, 3):
                far_copy(p, s, by).start()

    def sum_far(p, s):
        @pl.when(core == SUMMING)
        def _():
            whole_of(far.at[p, s], far_send.at[0], far_recv.at[p, s]).wait_recv()
            coefs[p, s, part_of(my_quarter)] = (near_sum[p, s] + far[p, s, 1]) + (far[p, s, 0] + far[p, s, 2])
            for by in (2, 1, 3):
                spread_copy(p, s, by, 1 - SUMMING).start()
                spread_copy(p, s, by, SUMMING).start()
            spread_copy(p, s, 0, 1 - SUMMING).start()

    def update(p, s):
        @pl.when(core == SUMMING)
        def _():
            whole_of(near.at[p, s, pl.ds(0, 3)], spread_send.at[0], spread_recv.at[p, s]).wait_recv()

        @pl.when(core != SUMMING)
        def _():
            whole_of(near.at[p, s, pl.ds(0, 4)], spread_send.at[0], spread_recv.at[p, s]).wait_recv()

        scaled = product(coefs[p, s], t_high[p], t_low[p], 0)
        x_turned[columns(s), :] = x_turned[columns(s), :] - product(scaled, w_high[p], w_low[p], 0)

    with scope("g0"):
        gather_0(last)
        announce(0)
        load_x = pltpu.make_async_copy(x_ref, x_in, load_sem.at[2 * panels])
        load_x.start()
        later_loads = [copy for p in range(last - 1, -1, -1) for copy in load(p)]
        load_x.wait()
        x_turned[...] = x_in[...].T
    with scope("g1"):
        gather_1(last)
        heard(0)
        announce(1)
    with scope("g2"):
        gather_2(last)
        heard(1)
        announce(2)
    with scope("g3"):
        gather_3(last)
        for copy in later_loads:
            copy.wait()
        gather_0(last - 1)
    with scope("g4"):
        gather_4(last)
        heard(2)
    with scope("prep"):
        split_panel(last)
    for s in range(STREAMS):
        with scope("project"):
            project(last, s)
    with scope("g1n"):
        gather_1(last - 1)
    for p in range(last, -1, -1):
        if p == 0:
            with scope("alone"):
                alone_wait().wait_recv()
                factor_copy(ALONE).start()
        if p > 0:
            with scope("turn"):
                turn_panel(p)
        if p == 1:
            with scope("g2n"):
                gather_2(p - 1)
        for s in range(STREAMS):
            with scope(f"near{s}"):
                sum_near(p, s)
        if p == 0:
            with scope("turn"):
                turn_panel(p)
        if p > 0:
            if p > 1:
                with scope("g2n"):
                    gather_2(p - 1)
            with scope("g3n"):
                gather_3(p - 1)
                if p > 1:
                    gather_0(p - 2)
                else:
                    send_alone()
        for s in range(STREAMS):
            with scope(f"far{s}"):
                sum_far(p, s)
        if p > 0:
            with scope("g4n"):
                gather_4(p - 1)
                factor_copy(CARRIED[p - 1]).start()
            with scope("prepn"):
                split_panel(p - 1)
        if p > 1:
            with scope("g1n"):
                gather_1(p - 2)
        with scope("factor"):
            split_factor(p)
        for s in range(STREAMS):
            with scope(f"update{s}"):
                update(p, s)
            if p > 0:
                with scope("project"):
                    project(p - 1, s)
    with scope("out"):
        out_ref[...] = x_turned[...].T
    with scope("drain"):
        for p in range(panels):
            whole = blocks.at[p, pl.ds(0, 15), pl.ds(0, length_of(p)), :]
            pltpu.make_async_remote_copy(
                src_ref=whole, dst_ref=whole, send_sem=gather_send.at[p], recv_sem=gather_last.at[p],
                device_id={"core": 1 - core}, device_id_type=MESH,
            ).wait_send()
        to_core(other_t, other_t, 0, factor_recv.at[0]).wait_send()
        alone_wait().wait_send()
        @pl.when(core == SUMMING)
        def _():
            whole_of(near.at[:, :, pl.ds(0, 3)], near_send.at[0], near_recv.at[0, 0]).wait_send()
            whole_of(far, far_send.at[0], far_recv.at[0, 0]).wait_send()
            whole_of(near.at[:, :, pl.ds(0, 7)], spread_send.at[0], spread_recv.at[0, 0]).wait_send()

        @pl.when(core != SUMMING)
        def _():
            whole_of(near.at[:, :, pl.ds(0, 4)], near_send.at[0], near_recv.at[0, 0]).wait_send()


def per_device(vectors, reflectors, triangles):
    panels, rows, width = reflectors.shape
    length, count = vectors.shape
    turned = jnp.swapaxes(triangles, 1, 2)
    half = turned.shape[1] // 2
    part = count // STREAMS // 4
    f32, bf16 = jnp.float32, jnp.bfloat16
    dma = pltpu.SemaphoreType.DMA
    return pl.pallas_call(
        kernel,
        out_shape=jax.ShapeDtypeStruct(vectors.shape, f32),
        in_specs=[pl.BlockSpec(memory_space=pltpu.HBM)] * 3,
        out_specs=pl.BlockSpec(memory_space=pltpu.VMEM),
        scratch_shapes=[
            pltpu.VMEM((length, count), f32),
            pltpu.VMEM((count, length), f32),
            pltpu.VMEM((panels, 16, rows + half, width), f32),
            pltpu.VMEM((16, half, width), f32),
            pltpu.VMEM((panels, 16, half, width), f32),
            pltpu.VMEM((panels, 16 * rows, width), bf16),
            pltpu.VMEM((panels, 16 * rows, width), bf16),
            pltpu.VMEM((panels, width, 16 * rows), bf16),
            pltpu.VMEM((panels, width, 16 * rows), bf16),
            pltpu.VMEM((panels, width, width), bf16),
            pltpu.VMEM((panels, width, width), bf16),
            pltpu.VMEM((panels, STREAMS, 4 * part, width), f32),
            pltpu.VMEM((panels, STREAMS, 8, part, width), f32),
            pltpu.VMEM((panels, STREAMS, part, width), f32),
            pltpu.VMEM((panels, STREAMS, 3, part, width), f32),
            pltpu.VMEM((panels, STREAMS, 4 * part, width), f32),
            dma((2 * panels + 1,)), pltpu.SemaphoreType.REGULAR((3,)),
            dma((panels,)), dma((panels, 4)), dma((panels, 2)), dma((panels, 16)), dma((panels,)),
            dma((1,)), dma((1,)), dma((1,)), dma((panels,)), dma((1,)), dma((panels, STREAMS)),
            dma((1,)), dma((panels, STREAMS)), dma((1,)), dma((panels, STREAMS)),
        ],
        compiler_params=pltpu.CompilerParams(collective_id=0, has_side_effects=True, vmem_limit_bytes=36 * 2**20),
    )(*(pltpu.with_memory_space_constraint(a, pltpu.HBM) for a in (vectors, reflectors, turned)))


def solution(mesh):
    finer = Mesh(mesh.devices.reshape(16, 2, 4, 4), ("z", "core", "y", "x"))
    placed = (P(ROW, VEC), P(None, ROW + VEC, None), P(None, None, VEC))
    return jax.shard_map(
        per_device, mesh=finer, in_specs=placed, out_specs=P(ROW, VEC), check_vma=False
    )
```
